768 devices in a mesh: gx: 16 (over y, z_hi), gy: 4 (over x), gz: 12 (over z_lo, core).
Axes of the slice: x: 4, y: 8, z: 12 (z_hi: 2, z_lo: 6; z = z_hi * 6 + z_lo), core: 2. Of those that a mesh axis runs over, the one named last changes fastest.
Arguments:
- pressure_now: float32 [256, 128, 1536], P('gx', 'gy', 'gz'), may hold values from -6 to 6
- pressure_before: float32 [256, 128, 1536], P('gx', 'gy', 'gz'), may hold values from -6 to 6
- region_code: int32 [256, 128, 1536], P('gx', 'gy', 'gz'), may hold values from 0 to 7
- velocity: float32 [8], replicated, may hold values from 0.2 to 0.42
- wavelet: float32 [6, 16], replicated, may hold values from -6 to 6
- source_cell: int32 [16], replicated, may hold values from 0 to 50331647
Outputs:
- pressure: float32 [256, 128, 1536], P('gx', 'gy', 'gz')
- previous: float32 [256, 128, 1536], P('gx', 'gy', 'gz')
The draws below stay inside these ranges and needn't reach their ends.
Inputs may be any that keep to these rules, and one draw needn't show every extreme that they name: source_cell[s] is the flat index x * 128 * 1536 + y * 1536 + z of a grid cell; sources may share a cell.
All inputs are finite; a program needn't handle non-finite values.
Results may differ from the reference program's by a relative error of at most 0.00002.
Values sent between devices are 32-bit elements; how exact they have to be, the bound alone decides.
No kernel may reach another device: no remote copies, remote signals or barrier semaphores. Data moves between devices by JAX's collectives and lax.ppermute only.
A program may use at most 32 MiB of HBM per device.

```python
import math
import jax
import jax.numpy as jnp
from jax import lax

STEPS = 6
NSRC = 16
NREG = 8
NX = 256
NY = 128
NZ = 1536


def touch_ends(array, rng, least, top_value):
    extent = array.shape
    place = [jax.random.randint(jax.random.fold_in(rng, axis), (), 0, extent[axis]) for axis in range(len(extent))]
    array = array.at[tuple(place)].set(least)
    longest = extent.index(max(extent))
    place[longest] = (place[longest] + 1) % extent[longest]
    return array.at[tuple(place)].set(top_value)


def steps_of(rng, dims, cuts, low, largest):
    factor_of, own = 1.0, jax.random.fold_in(rng, 6)
    for position, blocks in cuts:
        steps = jnp.exp(jax.random.uniform(jax.random.fold_in(own, position), (blocks,), jnp.float32, low / len(cuts), largest / len(cuts)))
        factor_of = factor_of * jnp.repeat(steps, dims[position] // blocks).reshape([-1 if axis == position else 1 for axis in range(len(dims))])
    return factor_of


def noise(own_key, extent, spread, limit, split=(), dtype=jnp.bfloat16):
    level = steps_of(own_key, extent, split, -0.22, 0.18) if split else 1.0
    result = jax.random.normal(own_key, extent, jnp.float32) * spread * level
    return jnp.minimum(jnp.maximum(result, -limit), limit).astype(dtype)


def setup_inputs(seed: int = 0) -> dict:
    splits = jax.random.split(jax.random.key(seed), 7)
    return {
        "pressure_now": noise(splits[0], (NX, NY, NZ), 1.0, 6.0, ((0, 16), (1, 4), (2, 12)), jnp.float32),
        "pressure_before": noise(splits[1], (NX, NY, NZ), 1.0, 6.0, ((0, 16), (1, 4), (2, 12)), jnp.float32),
        "region_code": touch_ends(jax.random.randint(splits[2], (NX, NY, NZ), 0, NREG), jax.random.fold_in(splits[2], 1), 0, NREG - 1).astype(jnp.int32),
        "velocity": jnp.clip(jnp.exp(jax.random.uniform(splits[3], (NREG,), jnp.float32, math.log(0.2), math.log(0.42))), 0.2, 0.42),
        "wavelet": noise(splits[4], (STEPS, NSRC), 1.0, 6.0, (), jnp.float32),
        "source_cell": touch_ends(jax.random.randint(splits[5], (NSRC,), 0, NX * NY * NZ), jax.random.fold_in(splits[5], 1), 0, (NX * NY * NZ) - 1).astype(jnp.int32),
    }


CENTRE = -205.0 / 72.0
WEIGHTS = (8.0 / 5.0, -1.0 / 5.0, 8.0 / 315.0, -1.0 / 560.0)


def cut(field, start, size):
    return lax.slice(field, tuple(start), tuple(a + b for a, b in zip(start, size)))


def along(field, axis, start, size):
    total = None
    for step_k, weight in enumerate(WEIGHTS, 1):
        upper = list(start)
        upper[axis] = upper[axis] + step_k
        lower = list(start)
        lower[axis] = lower[axis] - step_k
        term = weight * (cut(field, upper, size) + cut(field, lower, size))
        total = term if total is None else total + term
    return total


def reference(pressure_now, pressure_before, region_code, velocity, wavelet, source_cell):
    size = pressure_now.shape
    speed = velocity[region_code]
    rate = speed * speed
    current = pressure_now
    before = pressure_before
    for step in range(STEPS):
        padded = jnp.pad(current, ((4, 4), (0, 0), (0, 0)), mode="wrap")
        padded = jnp.pad(padded, ((0, 0), (4, 4), (4, 4)))
        start = (4, 4, 4)
        laplace = 3.0 * CENTRE * current + along(padded, 0, start, size) + along(padded, 1, start, size) + along(padded, 2, start, size)
        following = 2.0 * current - before + rate * laplace
        following = following.reshape(-1).at[source_cell].add(wavelet[step]).reshape(size)
        before = current
        current = following
    return current, before
```

```python
import jax
import jax.numpy as jnp
from jax import lax
from jax.experimental import pallas as pl
from jax.experimental.pallas import tpu as pltpu
from jax.sharding import PartitionSpec as P


STEPS = 6
CENTRE = -205.0 / 72.0
WEIGHTS = (8.0 / 5.0, -1.0 / 5.0, 8.0 / 315.0, -1.0 / 560.0)
HALO = 4
VMEM = pl.BlockSpec(memory_space=pltpu.VMEM)
SMEM = pl.BlockSpec(memory_space=pltpu.SMEM)


def banded(rows, columns, shift):
    i = lax.broadcasted_iota(jnp.int32, (rows, columns), 0) + shift
    j = lax.broadcasted_iota(jnp.int32, (rows, columns), 1)
    distance = jnp.abs(i - j)
    matrix = jnp.zeros((rows, columns), jnp.float32)
    for k, weight in enumerate(WEIGHTS, 1):
        matrix = jnp.where(distance == k, jnp.float32(weight), matrix)
    return matrix


def pack_faces(field_ref, faces):
    x_low, x_high, y_low, y_high, z_low, z_high = faces
    nx, ny, nz = field_ref.shape
    x_low[...] = field_ref[0:HALO]
    x_high[...] = field_ref[nx - HALO : nx]
    for x in range(nx):
        rows = slice(HALO * x, HALO * (x + 1))
        y_low[rows, :] = field_ref[x, 0:HALO, :]
        y_high[rows, :] = field_ref[x, ny - HALO : ny, :]
    rows = lax.broadcasted_iota(jnp.int32, (2 * HALO, nz), 0)
    lanes = lax.broadcasted_iota(jnp.int32, (2 * HALO, nz), 1)
    wanted = jnp.where(rows < HALO, rows, rows + nz - 2 * HALO)
    select = jnp.where(lanes == wanted, jnp.float32(1), jnp.float32(0))
    packed = lax.dot_general(
        select,
        field_ref[...].reshape(nx * ny, nz),
        (((1,), (1,)), ((), ())),
        precision=lax.Precision.HIGHEST,
        preferred_element_type=jnp.float32,
    )
    z_low[...] = packed[0:HALO]
    z_high[...] = packed[HALO : 2 * HALO]


def face_kernel(field_ref, *faces):
    pack_faces(field_ref, faces)


def step_kernel(last, places, amounts, now, before, rate, x_low, x_high, y_low, y_high, z_low, z_high, *rest):
    following = rest[0]
    faces = rest[1:-1]
    wide = rest[-1]
    nx, ny, nz = now.shape
    for x in range(nx):
        rows = slice(HALO * x, HALO * (x + 1))
        wide[x, 4:8, :] = y_low[rows, :]
        wide[x, 8 : 8 + ny, :] = now[x]
        wide[x, 8 + ny : 12 + ny, :] = y_high[rows, :]
    flat = now[...].reshape(nx * ny, nz)
    along_z = lax.dot_general(
        flat,
        banded(nz, nz, 0),
        (((1,), (0,)), ((), ())),
        precision=lax.Precision.HIGHEST,
        preferred_element_type=jnp.float32,
    )
    halo = jnp.concatenate([z_low[...], z_high[...]], axis=0)
    i = lax.broadcasted_iota(jnp.int32, (2 * HALO, nz), 0)
    j = lax.broadcasted_iota(jnp.int32, (2 * HALO, nz), 1)
    place = jnp.where(i < HALO, i - HALO, i - HALO + nz)
    distance = jnp.abs(place - j)
    weights = jnp.zeros((2 * HALO, nz), jnp.float32)
    for k, weight in enumerate(WEIGHTS, 1):
        weights = jnp.where(distance == k, jnp.float32(weight), weights)
    along_z += lax.dot_general(
        halo,
        weights,
        (((0,), (0,)), ((), ())),
        precision=lax.Precision.HIGHEST,
        preferred_element_type=jnp.float32,
    )
    along_z = along_z.reshape(nx, ny, nz)

    def layer(x):
        if x < 0:
            return x_low[x + HALO]
        if x >= nx:
            return x_high[x - nx]
        return now[x]

    for x in range(nx):
        here = now[x]
        total = jnp.float32(3.0 * CENTRE) * here + along_z[x]
        for k, weight in enumerate(WEIGHTS, 1):
            around = (layer(x + k) + layer(x - k)) + (
                wide[x, 8 + k : 8 + k + ny, :] + wide[x, 8 - k : 8 - k + ny, :]
            )
            total = total + jnp.float32(weight) * around
        following[x] = 2.0 * here - before[x] + rate[x] * total

    sources = amounts.shape[0]

    @pl.when(places[3, sources] > 0)
    def _():
        lanes = lax.broadcasted_iota(jnp.int32, (1, nz), 1)
        for s in range(sources):

            @pl.when(places[3, s] > 0)
            def _():
                x, y, z = places[0, s], places[1, s], places[2, s]
                row = following[x, pl.ds(y, 1), :]
                following[x, pl.ds(y, 1), :] = row + jnp.where(lanes == z, amounts[s], jnp.float32(0))

    if not last:
        pack_faces(following, faces)


def face_shapes(shape):
    nx, ny, nz = shape
    return (
        (HALO, ny, nz),
        (HALO, ny, nz),
        (HALO * nx, nz),
        (HALO * nx, nz),
        (HALO, nx * ny),
        (HALO, nx * ny),
    )


def arrays(shapes):
    return tuple(jax.ShapeDtypeStruct(s, jnp.float32) for s in shapes)


PARAMS = dict(vmem_limit_bytes=16 * 1024 * 1024)


def faces_of(field):
    shapes = face_shapes(field.shape)
    return pl.pallas_call(
        face_kernel,
        out_shape=arrays(shapes),
        in_specs=[VMEM],
        out_specs=(VMEM,) * 6,
        compiler_params=pltpu.CompilerParams(**PARAMS),
        cost_estimate=pl.CostEstimate(flops=2000000, bytes_accessed=600000, transcendentals=0),
        name="faces",
    )(field)


def advance(last, places, amounts, now, before, rate, halos):
    shape = now.shape
    nx, ny, nz = shape
    shapes = (shape,) if last else (shape,) + face_shapes(shape)
    out = pl.pallas_call(
        lambda *refs: step_kernel(last, *refs),
        out_shape=arrays(shapes),
        in_specs=[SMEM, SMEM] + [VMEM] * 9,
        out_specs=(VMEM,) * len(shapes),
        scratch_shapes=[pltpu.VMEM((nx, ny + 16, nz), jnp.float32)],
        compiler_params=pltpu.CompilerParams(**PARAMS),
        cost_estimate=pl.CostEstimate(flops=10000000, bytes_accessed=1500000, transcendentals=0),
        name="advance",
    )(places, amounts, now, before, rate, *halos)
    return out[0], out[1:]


def rates(codes, velocity):
    speed = jnp.zeros(codes.shape, jnp.float32)
    for region in range(velocity.shape[0]):
        speed = jnp.where(codes == region, velocity[region], speed)
    return speed * speed


def ring(count):
    return [(i, (i + 1) % count) for i in range(count)]


def line(count):
    return [(i, i + 1) for i in range(count - 1)]


def back(pairs):
    return [(b, a) for a, b in pairs]


def exchange(faces):
    x_low, x_high, y_low, y_high, z_low, z_high = faces
    up = ring(lax.axis_size("gx"))
    from_x_low = lax.ppermute(x_high, "gx", up)
    from_x_high = lax.ppermute(x_low, "gx", back(up))
    up = line(lax.axis_size("gy"))
    from_y_low = lax.ppermute(y_high, "gy", up)
    from_y_high = lax.ppermute(y_low, "gy", back(up))
    up = line(lax.axis_size("gz"))
    from_z_low = lax.ppermute(z_high, "gz", up)
    from_z_high = lax.ppermute(z_low, "gz", back(up))
    return from_x_low, from_x_high, from_y_low, from_y_high, from_z_low, from_z_high


def per_device(pressure_now, pressure_before, region_code, velocity, wavelet, source_cell):
    nx, ny, nz = pressure_now.shape
    grid_y = ny * lax.axis_size("gy")
    grid_z = nz * lax.axis_size("gz")
    x = source_cell // (grid_y * grid_z) - lax.axis_index("gx") * nx
    y = source_cell // grid_z % grid_y - lax.axis_index("gy") * ny
    z = source_cell % grid_z - lax.axis_index("gz") * nz
    inside = (x >= 0) & (x < nx) & (y >= 0) & (y < ny) & (z >= 0) & (z < nz)
    places = jnp.stack(
        [
            jnp.clip(x, 0, nx - 1),
            jnp.clip(y, 0, ny - 1),
            jnp.clip(z, 0, nz - 1),
            inside.astype(jnp.int32),
        ]
    )
    count = jnp.sum(places[3:4], axis=1, keepdims=True)
    places = jnp.concatenate([places, jnp.broadcast_to(count, (4, 1))], axis=1)

    rate = rates(region_code, velocity)
    current, before = pressure_now, pressure_before
    faces = faces_of(current)
    for step in range(STEPS):
        halos = exchange(faces)
        following, faces = advance(step == STEPS - 1, places, wavelet[step], current, before, rate, halos)
        before, current = current, following
    return current, before


def solution(mesh):
    field = P("gx", "gy", "gz")
    return jax.shard_map(
        per_device,
        mesh=mesh,
        in_specs=(field, field, field, P(), P(), P()),
        out_specs=(field, field),
        check_vma=False,
    )
```

```python
import jax
import jax.numpy as jnp
from jax import lax
from jax.experimental import pallas as pl
from jax.experimental.pallas import tpu as pltpu
from jax.sharding import PartitionSpec as P


STEPS = 6
CENTRE = -205.0 / 72.0
WEIGHTS = (8.0 / 5.0, -1.0 / 5.0, 8.0 / 315.0, -1.0 / 560.0)
HALO = 4
VMEM = pl.BlockSpec(memory_space=pltpu.VMEM)
SMEM = pl.BlockSpec(memory_space=pltpu.SMEM)


def banded(rows, columns, shift):
    i = lax.broadcasted_iota(jnp.int32, (rows, columns), 0) + shift
    j = lax.broadcasted_iota(jnp.int32, (rows, columns), 1)
    distance = jnp.abs(i - j)
    matrix = jnp.zeros((rows, columns), jnp.float32)
    for k, weight in enumerate(WEIGHTS, 1):
        matrix = jnp.where(distance == k, jnp.float32(weight), matrix)
    return matrix


def pack_faces(field_ref, pair, y_low, y_high, z_low, z_high):
    nx, ny, nz = field_ref.shape
    odd = lax.axis_index("gx") % 2
    inner = (1 - odd) * (nx - HALO)
    outer = odd * (nx - HALO)
    pair[0:HALO] = field_ref[pl.ds(inner, HALO)]
    pair[HALO : 2 * HALO] = field_ref[pl.ds(outer, HALO)]
    for x in range(nx):
        rows = slice(HALO * x, HALO * (x + 1))
        y_low[rows, :] = field_ref[x, 0:HALO, :]
        y_high[rows, :] = field_ref[x, ny - HALO : ny, :]
    rows = lax.broadcasted_iota(jnp.int32, (2 * HALO, nz), 0)
    lanes = lax.broadcasted_iota(jnp.int32, (2 * HALO, nz), 1)
    wanted = jnp.where(rows < HALO, rows, rows + nz - 2 * HALO)
    select = jnp.where(lanes == wanted, jnp.float32(1), jnp.float32(0))
    packed = lax.dot_general(
        select,
        field_ref[...].reshape(nx * ny, nz),
        (((1,), (1,)), ((), ())),
        precision=lax.Precision.HIGHEST,
        preferred_element_type=jnp.float32,
    )
    z_low[...] = packed[0:HALO]
    z_high[...] = packed[HALO : 2 * HALO]


def face_kernel(field_ref, *faces):
    pack_faces(field_ref, *faces)


def rate_kernel(velocity, codes, rate):
    regions = velocity.shape[0]
    squares = [velocity[r] * velocity[r] for r in range(regions)]
    for x in range(codes.shape[0]):
        code = codes[x]
        value = jnp.full(code.shape, squares[0], jnp.float32)
        for r in range(1, regions):
            value = jnp.where(code == r, squares[r], value)
        rate[x] = value


def step_kernel(last, now, before, rate, cells, amounts, inner, outer, y_low, y_high, z_low, z_high, *rest):
    following = rest[0]
    faces = rest[1:-2]
    wide, x_halo = rest[-2:]
    nx, ny, nz = now.shape
    odd = lax.axis_index("gx") % 2
    x_halo[pl.ds((1 - odd) * HALO, HALO)] = inner[...]
    x_halo[pl.ds(odd * HALO, HALO)] = outer[...]
    for x in range(nx):
        rows = slice(HALO * x, HALO * (x + 1))
        wide[x, 4:8, :] = y_low[rows, :]
        wide[x, 8 : 8 + ny, :] = now[x]
        wide[x, 8 + ny : 12 + ny, :] = y_high[rows, :]
    flat = now[...].reshape(nx * ny, nz)
    along_z = lax.dot_general(
        flat,
        banded(nz, nz, 0),
        (((1,), (0,)), ((), ())),
        precision=lax.Precision.HIGHEST,
        preferred_element_type=jnp.float32,
    )
    halo = jnp.concatenate([z_low[...], z_high[...]], axis=0)
    i = lax.broadcasted_iota(jnp.int32, (2 * HALO, nz), 0)
    j = lax.broadcasted_iota(jnp.int32, (2 * HALO, nz), 1)
    place = jnp.where(i < HALO, i - HALO, i - HALO + nz)
    distance = jnp.abs(place - j)
    weights = jnp.zeros((2 * HALO, nz), jnp.float32)
    for k, weight in enumerate(WEIGHTS, 1):
        weights = jnp.where(distance == k, jnp.float32(weight), weights)
    along_z += lax.dot_general(
        halo,
        weights,
        (((0,), (0,)), ((), ())),
        precision=lax.Precision.HIGHEST,
        preferred_element_type=jnp.float32,
    )
    along_z = along_z.reshape(nx, ny, nz)

    def layer(x):
        if x < 0:
            return x_halo[x + HALO]
        if x >= nx:
            return x_halo[x - nx + HALO]
        return now[x]

    for x in range(nx):
        here = now[x]
        total = jnp.float32(3.0 * CENTRE) * here + along_z[x]
        for k, weight in enumerate(WEIGHTS, 1):
            around = (layer(x + k) + layer(x - k)) + (
                wide[x, 8 + k : 8 + k + ny, :] + wide[x, 8 - k : 8 - k + ny, :]
            )
            total = total + jnp.float32(weight) * around
        following[x] = 2.0 * here - before[x] + rate[x] * total

    @pl.when(jnp.max(cells[...]) >= 0)
    def _():
        flat_index = lax.broadcasted_iota(jnp.int32, (ny, nz), 0) * nz + lax.broadcasted_iota(jnp.int32, (ny, nz), 1)

        def add(x, carry):
            index = flat_index + x * (ny * nz)
            total = following[x]
            for s in range(cells.shape[0]):
                total = total + jnp.where(index == cells[s : s + 1, :], amounts[s : s + 1, :], jnp.float32(0))
            following[x] = total
            return carry

        lax.fori_loop(0, nx, add, 0)

    if not last:
        pack_faces(following, *faces)


def face_shapes(shape):
    nx, ny, nz = shape
    return (
        (2 * HALO, ny, nz),
        (HALO * nx, nz),
        (HALO * nx, nz),
        (HALO, nx * ny),
        (HALO, nx * ny),
    )


def arrays(shapes):
    return tuple(jax.ShapeDtypeStruct(s, jnp.float32) for s in shapes)


PARAMS = dict(vmem_limit_bytes=16 * 1024 * 1024)


def faces_of(field):
    shapes = face_shapes(field.shape)
    return pl.pallas_call(
        face_kernel,
        out_shape=arrays(shapes),
        in_specs=[VMEM],
        out_specs=(VMEM,) * len(shapes),
        compiler_params=pltpu.CompilerParams(**PARAMS),
        cost_estimate=pl.CostEstimate(flops=2000000, bytes_accessed=600000, transcendentals=0),
        name="faces",
    )(field)


def rate_of(codes, velocity):
    return pl.pallas_call(
        rate_kernel,
        out_shape=jax.ShapeDtypeStruct(codes.shape, jnp.float32),
        in_specs=[SMEM, VMEM],
        out_specs=VMEM,
        compiler_params=pltpu.CompilerParams(**PARAMS),
        cost_estimate=pl.CostEstimate(flops=2000000, bytes_accessed=600000, transcendentals=0),
        name="rate",
    )(velocity, codes)


def advance(last, now, before, rate, cells, amounts, halos):
    shape = now.shape
    nx, ny, nz = shape
    shapes = (shape,) if last else (shape,) + face_shapes(shape)
    out = pl.pallas_call(
        lambda *refs: step_kernel(last, *refs),
        out_shape=arrays(shapes),
        in_specs=[VMEM] * 11,
        out_specs=(VMEM,) * len(shapes),
        scratch_shapes=[
            pltpu.VMEM((nx, ny + 16, nz), jnp.float32),
            pltpu.VMEM((2 * HALO, ny, nz), jnp.float32),
        ],
        compiler_params=pltpu.CompilerParams(**PARAMS),
        cost_estimate=pl.CostEstimate(flops=10000000, bytes_accessed=1500000, transcendentals=0),
        name="advance",
    )(now, before, rate, cells, amounts, *halos)
    return out[0], out[1:]


def line(count):
    return [(i, i + 1) for i in range(count - 1)]


def back(pairs):
    return [(b, a) for a, b in pairs]


def exchange(faces):
    pair, y_low, y_high, z_low, z_high = faces
    count = lax.axis_size("gx")
    swapped = lax.ppermute(pair, "gx", [(i, i ^ 1) for i in range(count)])
    up = line(lax.axis_size("gy"))
    from_y_low = lax.ppermute(y_high, "gy", up)
    from_y_high = lax.ppermute(y_low, "gy", back(up))
    up = line(lax.axis_size("gz"))
    from_z_low = lax.ppermute(z_high, "gz", up)
    from_z_high = lax.ppermute(z_low, "gz", back(up))
    swapped, from_y_low, from_y_high, from_z_low, from_z_high = lax.optimization_barrier(
        (swapped, from_y_low, from_y_high, from_z_low, from_z_high)
    )
    onward = [(i, (i + 2 - 4 * (i % 2)) % count) for i in range(count)]
    outer = lax.ppermute(swapped[HALO:], "gx", onward)
    return swapped[:HALO], outer, from_y_low, from_y_high, from_z_low, from_z_high


def per_device(pressure_now, pressure_before, region_code, velocity, wavelet, source_cell):
    nx, ny, nz = pressure_now.shape
    grid_y = ny * lax.axis_size("gy")
    grid_z = nz * lax.axis_size("gz")
    x = source_cell // (grid_y * grid_z) - lax.axis_index("gx") * nx
    y = source_cell // grid_z % grid_y - lax.axis_index("gy") * ny
    z = source_cell % grid_z - lax.axis_index("gz") * nz
    inside = (x >= 0) & (x < nx) & (y >= 0) & (y < ny) & (z >= 0) & (z < nz)
    cells = jnp.where(inside, (x * ny + y) * nz + z, -1)
    cells = jnp.broadcast_to(cells[:, None], (cells.shape[0], nz))
    amounts = [jnp.broadcast_to(wavelet[step][:, None], (wavelet.shape[1], nz)) for step in range(STEPS)]
    rate = rate_of(region_code, velocity)
    rate, cells, *amounts = lax.optimization_barrier((rate, cells, *amounts))
    current, before = pressure_now, pressure_before
    faces = faces_of(current)
    for step in range(STEPS):
        halos = exchange(faces)
        following, faces = advance(step == STEPS - 1, current, before, rate, cells, amounts[step], halos)
        before, current = current, following
    return current, before


def solution(mesh):
    field = P("gx", "gy", "gz")
    return jax.shard_map(
        per_device,
        mesh=mesh,
        in_specs=(field, field, field, P(), P(), P()),
        out_specs=(field, field),
        check_vma=False,
    )
```

```python
import jax
import jax.numpy as jnp
from jax import lax
from jax.experimental import pallas as pl
from jax.experimental.pallas import tpu as pltpu
from jax.sharding import PartitionSpec as P


STEPS = 6
CENTRE = -205.0 / 72.0
WEIGHTS = (8.0 / 5.0, -1.0 / 5.0, 8.0 / 315.0, -1.0 / 560.0)
HALO = 4
DEEP = HALO * STEPS
VMEM = pl.BlockSpec(memory_space=pltpu.VMEM)
SMEM = pl.BlockSpec(memory_space=pltpu.SMEM)


def extra(step):
    return DEEP - HALO * (step + 1)


def matmul(a, b, contract):
    return lax.dot_general(
        a, b, (contract, ((), ())), precision=lax.Precision.HIGHEST, preferred_element_type=jnp.float32
    )


def chosen(columns, nz):
    row = lax.broadcasted_iota(jnp.int32, (2 * columns, nz), 0)
    lane = lax.broadcasted_iota(jnp.int32, (2 * columns, nz), 1)
    wanted = jnp.where(row < columns, row, row + nz - 2 * columns)
    return jnp.where(lane == wanted, jnp.float32(1), jnp.float32(0))


def packed(rows, columns):
    return matmul(chosen(columns, rows.shape[1]), rows, ((1,), (1,)))


def unpacked(block, columns, nz):
    return matmul(block, chosen(columns, nz), ((0,), (0,)))


def pack_faces(field, columns, pair, y_low, y_high, rows):
    _, nx, ny, nz = field.shape
    odd = lax.axis_index("gx") % 2
    inner = (1 - odd) * (nx - HALO)
    outer = odd * (nx - HALO)
    face = HALO * ny
    for place, first in ((0, inner), (face + 2 * columns, outer)):
        pair[place : place + face, :] = field[0, pl.ds(first, HALO)].reshape(face, nz)
        if columns:
            pair[place + face : place + face + 2 * columns, :] = packed(
                field[1, pl.ds(first, HALO)].reshape(face, nz), columns
            )
    for y_face, y in ((y_low, 0), (y_high, ny - HALO)):
        for x in range(nx):
            y_face[HALO * x : HALO * (x + 1), :] = field[0, x, y : y + HALO, :]
        if columns:
            for x in range(nx):
                rows[HALO * x : HALO * (x + 1), :] = field[1, x, y : y + HALO, :]
            y_face[HALO * nx : HALO * nx + 2 * columns, 0 : HALO * nx] = packed(rows[...], columns)


def first_kernel(velocity, now, before, codes, rate, z_low, z_high):
    nx, ny, nz = now.shape
    regions = velocity.shape[0]
    squares = [velocity[r] * velocity[r] for r in range(regions)]
    for x in range(nx):
        code = codes[x]
        value = jnp.full(code.shape, squares[0], jnp.float32)
        for r in range(1, regions):
            value = jnp.where(code == r, squares[r], value)
        rate[x] = value
    for place, field in enumerate((now, before, rate)):
        both = packed(field[...].reshape(nx * ny, nz), DEEP)
        z_low[place * DEEP : (place + 1) * DEEP, :] = both[0:DEEP]
        z_high[place * DEEP : (place + 1) * DEEP, :] = both[DEEP : 2 * DEEP]


def widen_kernel(now, before, rate, from_low, from_high, wide_now, wide_before, wide_rate, pair, y_low, y_high, rows):
    nx, ny, nz = now.shape
    for place, (field, wide) in enumerate(((now, wide_now), (before, wide_before), (rate, wide_rate))):
        wide[0] = field[...]
        part = slice(place * DEEP, (place + 1) * DEEP)
        block = jnp.concatenate([from_high[part, :], from_low[part, :]], axis=0)
        wide[1] = unpacked(block, DEEP, nz).reshape(nx, ny, nz)
    pack_faces(wide_now, extra(0), pair, y_low, y_high, rows)


def part_one(step, now, before, rate, y_low, y_high, *rest):
    following, wide = rest[0], rest[-1]
    columns = extra(step)
    tiles = 2 if columns else 1
    _, nx, ny, nz = now.shape
    for t in range(tiles):
        for place, y_face in ((8 - HALO, y_low), (8 + ny, y_high)):
            if t == 0:
                face = y_face[0 : HALO * nx, :]
            else:
                face = unpacked(y_face[HALO * nx : HALO * nx + 2 * columns, 0 : HALO * nx], columns, nz)
            for x in range(nx):
                wide[t, x, place : place + HALO, :] = face[HALO * x : HALO * (x + 1), :]
        for x in range(nx):
            wide[t, x, 8 : 8 + ny, :] = now[t, x]
    both = jnp.concatenate([now[0].reshape(nx * ny, nz), now[1].reshape(nx * ny, nz)], axis=1)
    i = lax.broadcasted_iota(jnp.int32, (2 * nz, tiles * nz), 0)
    j = lax.broadcasted_iota(jnp.int32, (2 * nz, tiles * nz), 1)
    distance = jnp.abs(i - j)
    distance = jnp.minimum(distance, 2 * nz - distance)
    band = jnp.zeros(distance.shape, jnp.float32)
    for k, weight in enumerate(WEIGHTS, 1):
        band = jnp.where(distance == k, jnp.float32(weight), band)
    along_z = matmul(both, band, ((1,), (0,)))
    for t in range(tiles):
        mine = along_z[:, t * nz : (t + 1) * nz].reshape(nx, ny, nz)
        for x in range(nx):
            here = now[t, x]
            total = jnp.float32(3.0 * CENTRE) * here + mine[x]
            for k, weight in enumerate(WEIGHTS, 1):
                around = wide[t, x, 8 + k : 8 + k + ny, :] + wide[t, x, 8 - k : 8 - k + ny, :]
                if x + k < nx:
                    around = around + now[t, x + k]
                if x - k >= 0:
                    around = around + now[t, x - k]
                total = total + jnp.float32(weight) * around
            value = 2.0 * here - before[t, x] + rate[t, x] * total
            if tiles == 2:
                following[t, x] = value
            else:
                following[x] = value
    if tiles == 1:
        rest[1][...] = now[0]


def part_two(step, partial, rate, cells, amounts, inner, outer, following, *rest):
    columns = extra(step)
    tiles = 2 if columns else 1
    _, nx, ny, nz = rate.shape
    if tiles == 2:
        pair, y_low, y_high, halo, rows = rest
    else:
        (halo,) = rest
    odd = lax.axis_index("gx") % 2
    face = HALO * ny
    for block, first in ((inner, (1 - odd) * HALO), (outer, odd * HALO)):
        halo[0, pl.ds(first, HALO)] = block[0:face, :].reshape(HALO, ny, nz)
        if columns:
            halo[1, pl.ds(first, HALO)] = unpacked(block[face : face + 2 * columns, :], columns, nz).reshape(HALO, ny, nz)
    for t in range(tiles):
        for x in range(nx):
            total = None
            for k, weight in enumerate(WEIGHTS, 1):
                for at in (x - k, x + k):
                    if 0 <= at < nx:
                        continue
                    term = jnp.float32(weight) * halo[t, at + HALO if at < 0 else at - nx + HALO]
                    total = term if total is None else total + term
            if tiles == 2:
                value = partial[t, x]
            else:
                value = partial[x]
            if total is not None:
                value = value + rate[t, x] * total
            if tiles == 2:
                following[t, x] = value
            else:
                following[x] = value

    @pl.when(jnp.max(cells[...]) >= 0)
    def _():
        flat_index = lax.broadcasted_iota(jnp.int32, (ny, nz), 0) * nz + lax.broadcasted_iota(jnp.int32, (ny, nz), 1)

        def add(n, carry):
            index = flat_index + n * (ny * nz)
            if tiles == 2:
                here = following.at[n // nx, n % nx]
            else:
                here = following.at[n]
            total = here[...]
            for s in range(cells.shape[0]):
                total = total + jnp.where(index == cells[s : s + 1, :], amounts[s : s + 1, :], jnp.float32(0))
            here[...] = total
            return carry

        lax.fori_loop(0, tiles * nx, add, 0)

    if tiles == 2:
        pack_faces(following, extra(step + 1), pair, y_low, y_high, rows)


def arrays(*shapes):
    return tuple(jax.ShapeDtypeStruct(s, jnp.float32) for s in shapes)


def face_shapes(shape, columns):
    nx, ny, nz = shape
    return (
        (2 * (HALO * ny + 2 * columns), nz),
        (HALO * nx + 2 * columns, nz),
        (HALO * nx + 2 * columns, nz),
    )


def call(kernel, name, out, inputs, operands, scratch=(), aliases=None):
    return pl.pallas_call(
        kernel,
        out_shape=out,
        in_specs=inputs,
        out_specs=(VMEM,) * len(out),
        scratch_shapes=[pltpu.VMEM(s, jnp.float32) for s in scratch],
        input_output_aliases=aliases or {},
        compiler_params=pltpu.CompilerParams(vmem_limit_bytes=16 * 1024 * 1024),
        cost_estimate=pl.CostEstimate(flops=5000000, bytes_accessed=1500000, transcendentals=0),
        name=name,
    )(*operands)


def line(count):
    return [(i, i + 1) for i in range(count - 1)]


def back(pairs):
    return [(b, a) for a, b in pairs]


def exchange(faces, ny, columns):
    pair, y_low, y_high = faces
    half = HALO * ny + 2 * columns
    count = lax.axis_size("gx")
    swapped = lax.ppermute(pair, "gx", [(i, i ^ 1) for i in range(count)])
    up = line(lax.axis_size("gy"))
    from_y_low = lax.ppermute(y_high, "gy", up)
    from_y_high = lax.ppermute(y_low, "gy", back(up))
    swapped, from_y_low, from_y_high = lax.optimization_barrier((swapped, from_y_low, from_y_high))
    onward = [(i, (i + 2 - 4 * (i % 2)) % count) for i in range(count)]
    outer = lax.ppermute(swapped[half:], "gx", onward)
    return swapped[:half], outer, from_y_low, from_y_high


def per_device(pressure_now, pressure_before, region_code, velocity, wavelet, source_cell):
    shape = pressure_now.shape
    nx, ny, nz = shape
    field = (2,) + shape
    rows = (HALO * nx, nz)
    grid_y = ny * lax.axis_size("gy")
    grid_z = nz * lax.axis_size("gz")
    x = source_cell // (grid_y * grid_z) - lax.axis_index("gx") * nx
    y = source_cell // grid_z % grid_y - lax.axis_index("gy") * ny
    z = source_cell % grid_z - lax.axis_index("gz") * nz
    inside = (x >= 0) & (x < nx) & (y >= 0) & (y < ny) & (z >= -DEEP) & (z < nz + DEEP)
    place = jnp.where(z < 0, z + 2 * nz, z)
    cells = jnp.where(inside, (((place // nz) * nx + x) * ny + y) * nz + place % nz, -1)
    cells = jnp.broadcast_to(cells[:, None], (cells.shape[0], nz))
    amounts = [jnp.broadcast_to(wavelet[step][:, None], (wavelet.shape[1], nz)) for step in range(STEPS)]

    deep = (3 * DEEP, nx * ny)
    rate, z_low, z_high = call(
        first_kernel,
        "first",
        arrays(shape, deep, deep),
        [SMEM, VMEM, VMEM, VMEM],
        (velocity, pressure_now, pressure_before, region_code),
    )
    up = line(lax.axis_size("gz"))
    from_low = lax.ppermute(z_high, "gz", up)
    from_high = lax.ppermute(z_low, "gz", back(up))
    from_low, from_high, cells, *amounts = lax.optimization_barrier((from_low, from_high, cells, *amounts))
    current, before, rate, *faces = call(
        widen_kernel,
        "widen",
        arrays(field, field, field, *face_shapes(shape, extra(0))),
        [VMEM] * 5,
        (pressure_now, pressure_before, rate, from_low, from_high),
        scratch=[rows],
    )
    for step in range(STEPS):
        last = step == STEPS - 1
        inner, outer, y_low, y_high = exchange(faces, ny, extra(step))
        out = call(
            lambda *refs, step=step: part_one(step, *refs),
            "part_one",
            arrays(shape, shape) if last else arrays(field),
            [VMEM] * 5,
            (current, before, rate, y_low, y_high),
            scratch=[(2, nx, ny + 16, nz)],
        )
        partial = out[0]
        following, *faces = call(
            lambda *refs, step=step: part_two(step, *refs),
            "part_two",
            arrays(shape) if last else arrays(field, *face_shapes(shape, extra(step + 1))),
            [VMEM] * 6,
            (partial, rate, cells, amounts[step], inner, outer),
            scratch=[(2, 2 * HALO, ny, nz)] if last else [(2, 2 * HALO, ny, nz), rows],
        )
        before, current = (out[1], following) if last else (current, following)
    return current, before


def solution(mesh):
    field = P("gx", "gy", "gz")
    return jax.shard_map(
        per_device,
        mesh=mesh,
        in_specs=(field, field, field, P(), P(), P()),
        out_specs=(field, field),
        check_vma=False,
    )
```

```python
import jax
import jax.numpy as jnp
from jax import lax
from jax.experimental import pallas as pl
from jax.experimental.pallas import tpu as pltpu
from jax.sharding import PartitionSpec as P


STEPS = 6
CENTRE = -205.0 / 72.0
WEIGHTS = (8.0 / 5.0, -1.0 / 5.0, 8.0 / 315.0, -1.0 / 560.0)
HALO = 4
DEEP = HALO * STEPS
VMEM = pl.BlockSpec(memory_space=pltpu.VMEM)


def extra(step):
    return DEEP - HALO * (step + 1)


def matmul(a, b, contract):
    return lax.dot_general(
        a, b, (contract, ((), ())), precision=lax.Precision.HIGHEST, preferred_element_type=jnp.float32
    )


def chosen(columns, nz):
    row = lax.broadcasted_iota(jnp.int32, (2 * columns, nz), 0)
    lane = lax.broadcasted_iota(jnp.int32, (2 * columns, nz), 1)
    wanted = jnp.where(row < columns, row, row + nz - 2 * columns)
    return jnp.where(lane == wanted, jnp.float32(1), jnp.float32(0))


def packed(rows, columns):
    return matmul(chosen(columns, rows.shape[1]), rows, ((1,), (1,)))


def unpacked(block, columns, nz):
    return matmul(block, chosen(columns, nz), ((0,), (0,)))


def pack_faces(field, columns, pair, y_low, y_high, rows):
    _, nx, ny, nz = field.shape
    odd = lax.axis_index("gx") % 2
    inner = (1 - odd) * (nx - HALO)
    outer = odd * (nx - HALO)
    face = HALO * ny
    for place, first in ((0, inner), (face + 2 * columns, outer)):
        pair[place : place + face, :] = field[0, pl.ds(first, HALO)].reshape(face, nz)
        if columns:
            pair[place + face : place + face + 2 * columns, :] = packed(
                field[1, pl.ds(first, HALO)].reshape(face, nz), columns
            )
    for y_face, y in ((y_low, 0), (y_high, ny - HALO)):
        for x in range(nx):
            y_face[HALO * x : HALO * (x + 1), :] = field[0, x, y : y + HALO, :]
        if columns:
            for x in range(nx):
                rows[HALO * x : HALO * (x + 1), :] = field[1, x, y : y + HALO, :]
            y_face[HALO * nx : HALO * nx + 2 * columns, 0 : HALO * nx] = packed(rows[...], columns)


def first_kernel(velocity_in, now_in, before_in, codes_in, rate, z_low, z_high, velocity, now, before, codes, arrived):
    nx, ny, nz = now.shape
    regions = velocity.shape[0]
    copies = [
        pltpu.make_async_copy(source, target, arrived.at[n])
        for n, (source, target) in enumerate(
            ((velocity_in, velocity), (codes_in, codes), (now_in, now), (before_in, before))
        )
    ]
    for copy in copies:
        copy.start()
    copies[0].wait()
    copies[1].wait()
    squares = [velocity[r] * velocity[r] for r in range(regions)]
    for x in range(nx):
        code = codes[x]
        value = jnp.full(code.shape, squares[0], jnp.float32)
        for r in range(1, regions):
            value = jnp.where(code == r, squares[r], value)
        rate[x] = value
    copies[2].wait()
    copies[3].wait()
    for place, field in enumerate((now, before, rate)):
        both = packed(field[...].reshape(nx * ny, nz), DEEP)
        z_low[place * DEEP : (place + 1) * DEEP, :] = both[0:DEEP]
        z_high[place * DEEP : (place + 1) * DEEP, :] = both[DEEP : 2 * DEEP]


def widen_kernel(now, before, rate, from_low, from_high, wide_now, wide_before, wide_rate, pair, y_low, y_high, rows):
    nx, ny, nz = now.shape
    for place, (field, wide) in enumerate(((now, wide_now), (before, wide_before), (rate, wide_rate))):
        wide[0] = field[...]
        part = slice(place * DEEP, (place + 1) * DEEP)
        block = jnp.concatenate([from_high[part, :], from_low[part, :]], axis=0)
        wide[1] = unpacked(block, DEEP, nz).reshape(nx, ny, nz)
    pack_faces(wide_now, extra(0), pair, y_low, y_high, rows)


def part_one(step, now, before, rate, cells, amounts, y_low, y_high, *rest):
    following, wide = rest[0], rest[-1]
    columns = extra(step)
    tiles = 2 if columns else 1
    _, nx, ny, nz = now.shape
    for t in range(tiles):
        for place, y_face in ((8 - HALO, y_low), (8 + ny, y_high)):
            if t == 0:
                face = y_face[0 : HALO * nx, :]
            else:
                face = unpacked(y_face[HALO * nx : HALO * nx + 2 * columns, 0 : HALO * nx], columns, nz)
            for x in range(nx):
                wide[t, x, place : place + HALO, :] = face[HALO * x : HALO * (x + 1), :]
        for x in range(nx):
            wide[t, x, 8 : 8 + ny, :] = now[t, x]
    both = jnp.concatenate([now[0].reshape(nx * ny, nz), now[1].reshape(nx * ny, nz)], axis=1)
    i = lax.broadcasted_iota(jnp.int32, (2 * nz, tiles * nz), 0)
    j = lax.broadcasted_iota(jnp.int32, (2 * nz, tiles * nz), 1)
    distance = jnp.abs(i - j)
    distance = jnp.minimum(distance, 2 * nz - distance)
    band = jnp.zeros(distance.shape, jnp.float32)
    for k, weight in enumerate(WEIGHTS, 1):
        band = jnp.where(distance == k, jnp.float32(weight), band)
    along_z = matmul(both, band, ((1,), (0,)))
    for t in range(tiles):
        mine = along_z[:, t * nz : (t + 1) * nz].reshape(nx, ny, nz)
        for x in range(nx):
            here = now[t, x]
            total = jnp.float32(3.0 * CENTRE) * here + mine[x]
            for k, weight in enumerate(WEIGHTS, 1):
                around = wide[t, x, 8 + k : 8 + k + ny, :] + wide[t, x, 8 - k : 8 - k + ny, :]
                if x + k < nx:
                    around = around + now[t, x + k]
                if x - k >= 0:
                    around = around + now[t, x - k]
                total = total + jnp.float32(weight) * around
            value = 2.0 * here - before[t, x] + rate[t, x] * total
            if tiles == 2:
                following[t, x] = value
            else:
                following[x] = value
    if tiles == 1:
        rest[1][...] = now[0]

    @pl.when(jnp.max(cells[...]) >= 0)
    def _():
        lanes = lax.broadcasted_iota(jnp.int32, (1, nz), 1)
        numbers = [jnp.max(cells[s : s + 1, :]) for s in range(cells.shape[0])]
        for s, number in enumerate(numbers):

            @pl.when((number >= 0) & (number < tiles * nx * ny * nz))
            def _():
                line_of = number // nz
                y = line_of % ny
                x = line_of // ny % nx
                if tiles == 2:
                    here = following.at[line_of // (nx * ny), x]
                else:
                    here = following.at[x]
                row = here[pl.ds(y, 1), :]
                here[pl.ds(y, 1), :] = row + jnp.where(lanes == number % nz, amounts[s : s + 1, :], jnp.float32(0))


def part_two(step, partial, rate, inner, outer, following, *rest):
    columns = extra(step)
    tiles = 2 if columns else 1
    _, nx, ny, nz = rate.shape
    if tiles == 2:
        pair, y_low, y_high, halo, rows = rest
    else:
        (halo,) = rest
    odd = lax.axis_index("gx") % 2
    face = HALO * ny
    for block, first in ((inner, (1 - odd) * HALO), (outer, odd * HALO)):
        halo[0, pl.ds(first, HALO)] = block[0:face, :].reshape(HALO, ny, nz)
        if columns:
            halo[1, pl.ds(first, HALO)] = unpacked(block[face : face + 2 * columns, :], columns, nz).reshape(HALO, ny, nz)
    for t in range(tiles):
        for x in range(nx):
            total = None
            for k, weight in enumerate(WEIGHTS, 1):
                for at in (x - k, x + k):
                    if 0 <= at < nx:
                        continue
                    term = jnp.float32(weight) * halo[t, at + HALO if at < 0 else at - nx + HALO]
                    total = term if total is None else total + term
            value = partial[t, x] if tiles == 2 else partial[x]
            if total is not None:
                value = value + rate[t, x] * total
            if tiles == 2:
                following[t, x] = value
            else:
                following[x] = value

    if tiles == 2:
        pack_faces(following, extra(step + 1), pair, y_low, y_high, rows)


def arrays(*shapes):
    return tuple(jax.ShapeDtypeStruct(s, jnp.float32) for s in shapes)


def face_shapes(shape, columns):
    nx, ny, nz = shape
    return (
        (2 * (HALO * ny + 2 * columns), nz),
        (HALO * nx + 2 * columns, nz),
        (HALO * nx + 2 * columns, nz),
    )


def call(kernel, name, out, inputs, operands, scratch=()):
    return pl.pallas_call(
        kernel,
        out_shape=out,
        in_specs=inputs,
        out_specs=(VMEM,) * len(out),
        scratch_shapes=[pltpu.VMEM(s, jnp.float32) for s in scratch],
        compiler_params=pltpu.CompilerParams(vmem_limit_bytes=16 * 1024 * 1024),
        cost_estimate=pl.CostEstimate(flops=5000000, bytes_accessed=1500000, transcendentals=0),
        name=name,
    )(*operands)


def line(count):
    return [(i, i + 1) for i in range(count - 1)]


def back(pairs):
    return [(b, a) for a, b in pairs]


def exchange(faces, ny, columns):
    pair, y_low, y_high = faces
    half = HALO * ny + 2 * columns
    count = lax.axis_size("gx")
    swapped = lax.ppermute(pair, "gx", [(i, i ^ 1) for i in range(count)])
    up = line(lax.axis_size("gy"))
    from_y_low = lax.ppermute(y_high, "gy", up)
    from_y_high = lax.ppermute(y_low, "gy", back(up))
    swapped, from_y_low, from_y_high = lax.optimization_barrier((swapped, from_y_low, from_y_high))
    onward = [(i, (i + 2 - 4 * (i % 2)) % count) for i in range(count)]
    outer = lax.ppermute(swapped[half:], "gx", onward)
    return swapped[:half], outer, from_y_low, from_y_high


def per_device(pressure_now, pressure_before, region_code, velocity, wavelet, source_cell):
    shape = pressure_now.shape
    nx, ny, nz = shape
    field = (2,) + shape
    rows = (HALO * nx, nz)
    grid_y = ny * lax.axis_size("gy")
    grid_z = nz * lax.axis_size("gz")
    x = source_cell // (grid_y * grid_z) - lax.axis_index("gx") * nx
    y = source_cell // grid_z % grid_y - lax.axis_index("gy") * ny
    z = source_cell % grid_z - lax.axis_index("gz") * nz
    inside = (x >= 0) & (x < nx) & (y >= 0) & (y < ny) & (z >= -DEEP) & (z < nz + DEEP)
    place = jnp.where(z < 0, z + 2 * nz, z)
    cells = jnp.where(inside, (((place // nz) * nx + x) * ny + y) * nz + place % nz, -1)
    cells = jnp.broadcast_to(cells[:, None], (cells.shape[0], nz))
    amounts = [jnp.broadcast_to(wavelet[step][:, None], (wavelet.shape[1], nz)) for step in range(STEPS)]

    deep = (3 * DEEP, nx * ny)
    in_hbm = pl.BlockSpec(memory_space=pltpu.HBM)
    rate, z_low, z_high = pl.pallas_call(
        first_kernel,
        out_shape=arrays(shape, deep, deep),
        in_specs=[in_hbm] * 4,
        out_specs=(VMEM,) * 3,
        scratch_shapes=[
            pltpu.SMEM(velocity.shape, jnp.float32),
            pltpu.VMEM(shape, jnp.float32),
            pltpu.VMEM(shape, jnp.float32),
            pltpu.VMEM(shape, jnp.int32),
            pltpu.SemaphoreType.DMA((4,)),
        ],
        compiler_params=pltpu.CompilerParams(vmem_limit_bytes=16 * 1024 * 1024),
        cost_estimate=pl.CostEstimate(flops=5000000, bytes_accessed=1500000, transcendentals=0),
        name="first",
    )(*(pltpu.with_memory_space_constraint(a, pltpu.HBM) for a in (velocity, pressure_now, pressure_before, region_code)))
    up = line(lax.axis_size("gz"))
    from_low = lax.ppermute(z_high, "gz", up)
    from_high = lax.ppermute(z_low, "gz", back(up))
    from_low, from_high, cells, *amounts = lax.optimization_barrier((from_low, from_high, cells, *amounts))
    current, before, rate, *faces = call(
        widen_kernel,
        "widen",
        arrays(field, field, field, *face_shapes(shape, extra(0))),
        [VMEM] * 5,
        (pressure_now, pressure_before, rate, from_low, from_high),
        scratch=[rows],
    )
    for step in range(STEPS):
        last = step == STEPS - 1
        inner, outer, y_low, y_high = exchange(faces, ny, extra(step))
        out = call(
            lambda *refs, step=step: part_one(step, *refs),
            "part_one",
            arrays(shape, shape) if last else arrays(field),
            [VMEM] * 7,
            (current, before, rate, cells, amounts[step], y_low, y_high),
            scratch=[(2, nx, ny + 16, nz)],
        )
        partial = out[0]
        following, *faces = call(
            lambda *refs, step=step: part_two(step, *refs),
            "part_two",
            arrays(shape) if last else arrays(field, *face_shapes(shape, extra(step + 1))),
            [VMEM] * 4,
            (partial, rate, inner, outer),
            scratch=[(2, 2 * HALO, ny, nz)] if last else [(2, 2 * HALO, ny, nz), rows],
        )
        before, current = (out[1], following) if last else (current, following)
    return current, before


def solution(mesh):
    field = P("gx", "gy", "gz")
    return jax.shard_map(
        per_device,
        mesh=mesh,
        in_specs=(field, field, field, P(), P(), P()),
        out_specs=(field, field),
        check_vma=False,
    )
```

```python
import jax
import jax.numpy as jnp
from jax import lax
from jax.experimental import pallas as pl
from jax.experimental.pallas import tpu as pltpu
from jax.sharding import PartitionSpec as P


STEPS = 6
CENTRE = -205.0 / 72.0
WEIGHTS = (8.0 / 5.0, -1.0 / 5.0, 8.0 / 315.0, -1.0 / 560.0)
HALO = 4
DEEP = HALO * STEPS
VMEM = pl.BlockSpec(memory_space=pltpu.VMEM)


def extra(step):
    return DEEP - HALO * (step + 1)


def matmul(a, b, contract):
    return lax.dot_general(
        a, b, (contract, ((), ())), precision=lax.Precision.HIGHEST, preferred_element_type=jnp.float32
    )


def chosen(columns, nz):
    row = lax.broadcasted_iota(jnp.int32, (2 * columns, nz), 0)
    lane = lax.broadcasted_iota(jnp.int32, (2 * columns, nz), 1)
    wanted = jnp.where(row < columns, row, row + nz - 2 * columns)
    return jnp.where(lane == wanted, jnp.float32(1), jnp.float32(0))


def packed(rows, columns):
    return matmul(chosen(columns, rows.shape[1]), rows, ((1,), (1,)))


def unpacked(block, columns, nz):
    return matmul(block, chosen(columns, nz), ((0,), (0,)))


def pack_faces(field, columns, pair, y_low, y_high, rows):
    _, nx, ny, nz = field.shape
    odd = lax.axis_index("gx") % 2
    inner = (1 - odd) * (nx - HALO)
    outer = odd * (nx - HALO)
    face = HALO * ny
    for place, first in ((0, inner), (face + 2 * columns, outer)):
        pair[place : place + face, :] = field[0, pl.ds(first, HALO)].reshape(face, nz)
        if columns:
            pair[place + face : place + face + 2 * columns, :] = packed(
                field[1, pl.ds(first, HALO)].reshape(face, nz), columns
            )
    for y_face, y in ((y_low, 0), (y_high, ny - HALO)):
        for x in range(nx):
            y_face[HALO * x : HALO * (x + 1), :] = field[0, x, y : y + HALO, :]
        if columns:
            for x in range(nx):
                rows[HALO * x : HALO * (x + 1), :] = field[1, x, y : y + HALO, :]
            y_face[HALO * nx : HALO * nx + 2 * columns, 0 : HALO * nx] = packed(rows[...], columns)


def first_kernel(velocity_in, now_in, before_in, codes_in, rate, z_low, z_high, velocity, now, before, codes, arrived):
    nx, ny, nz = now.shape
    regions = velocity.shape[0]
    copies = [
        pltpu.make_async_copy(source, target, arrived.at[n])
        for n, (source, target) in enumerate(
            ((velocity_in, velocity), (codes_in, codes), (now_in, now), (before_in, before))
        )
    ]
    for copy in copies:
        copy.start()
    copies[0].wait()
    copies[1].wait()
    squares = [velocity[r] * velocity[r] for r in range(regions)]
    for x in range(nx):
        code = codes[x]
        value = jnp.full(code.shape, squares[0], jnp.float32)
        for r in range(1, regions):
            value = jnp.where(code == r, squares[r], value)
        rate[x] = value
    copies[2].wait()
    copies[3].wait()
    for place, field in enumerate((now, before, rate)):
        both = packed(field[...].reshape(nx * ny, nz), DEEP)
        z_low[place * DEEP : (place + 1) * DEEP, :] = both[0:DEEP]
        z_high[place * DEEP : (place + 1) * DEEP, :] = both[DEEP : 2 * DEEP]


def widen_kernel(now, before, rate, from_low, from_high, wide_now, wide_before, wide_rate, pair, y_low, y_high, rows):
    nx, ny, nz = now.shape
    for place, (field, wide) in enumerate(((now, wide_now), (before, wide_before), (rate, wide_rate))):
        wide[0] = field[...]
        part = slice(place * DEEP, (place + 1) * DEEP)
        block = jnp.concatenate([from_high[part, :], from_low[part, :]], axis=0)
        wide[1] = unpacked(block, DEEP, nz).reshape(nx, ny, nz)
    pack_faces(wide_now, extra(0), pair, y_low, y_high, rows)


def part_one(step, now, before, rate, cells, amounts, y_low, y_high, *rest):
    following, wide = rest[0], rest[-1]
    columns = extra(step)
    tiles = 2 if columns else 1
    _, nx, ny, nz = now.shape
    for t in range(tiles):
        for place, y_face in ((8 - HALO, y_low), (8 + ny, y_high)):
            if t == 0:
                face = y_face[0 : HALO * nx, :]
            else:
                face = unpacked(y_face[HALO * nx : HALO * nx + 2 * columns, 0 : HALO * nx], columns, nz)
            for x in range(nx):
                wide[t, x, place : place + HALO, :] = face[HALO * x : HALO * (x + 1), :]
        for x in range(nx):
            wide[t, x, 8 : 8 + ny, :] = now[t, x]
    both = jnp.concatenate([now[0].reshape(nx * ny, nz), now[1].reshape(nx * ny, nz)], axis=1)
    i = lax.broadcasted_iota(jnp.int32, (2 * nz, tiles * nz), 0)
    j = lax.broadcasted_iota(jnp.int32, (2 * nz, tiles * nz), 1)
    distance = jnp.abs(i - j)
    distance = jnp.minimum(distance, 2 * nz - distance)
    band = jnp.zeros(distance.shape, jnp.float32)
    for k, weight in enumerate(WEIGHTS, 1):
        band = jnp.where(distance == k, jnp.float32(weight), band)
    along_z = matmul(both, band, ((1,), (0,)))
    for t in range(tiles):
        mine = along_z[:, t * nz : (t + 1) * nz].reshape(nx, ny, nz)
        for x in range(nx):
            here = now[t, x]
            total = jnp.float32(3.0 * CENTRE) * here + mine[x]
            for k, weight in enumerate(WEIGHTS, 1):
                around = wide[t, x, 8 + k : 8 + k + ny, :] + wide[t, x, 8 - k : 8 - k + ny, :]
                if x + k < nx:
                    around = around + now[t, x + k]
                if x - k >= 0:
                    around = around + now[t, x - k]
                total = total + jnp.float32(weight) * around
            value = 2.0 * here - before[t, x] + rate[t, x] * total
            if tiles == 2:
                following[t, x] = value
            else:
                following[x] = value
    if tiles == 1:
        rest[1][...] = now[0]

    @pl.when(jnp.max(cells[...]) >= 0)
    def _():
        lanes = lax.broadcasted_iota(jnp.int32, (1, nz), 1)
        numbers = [jnp.max(cells[s : s + 1, :]) for s in range(cells.shape[0])]
        for s, number in enumerate(numbers):

            @pl.when((number >= 0) & (number < tiles * nx * ny * nz))
            def _():
                line_of = number // nz
                y = line_of % ny
                x = line_of // ny % nx
                if tiles == 2:
                    here = following.at[line_of // (nx * ny), x]
                else:
                    here = following.at[x]
                row = here[pl.ds(y, 1), :]
                here[pl.ds(y, 1), :] = row + jnp.where(lanes == number % nz, amounts[s : s + 1, :], jnp.float32(0))


def part_two(step, partial, rate, inner, outer, following, *rest):
    columns = extra(step)
    tiles = 2 if columns else 1
    _, nx, ny, nz = rate.shape
    if tiles == 2:
        pair, y_low, y_high, halo, rows = rest
    else:
        (halo,) = rest
    odd = lax.axis_index("gx") % 2
    face = HALO * ny
    for block, first in ((inner, (1 - odd) * HALO), (outer, odd * HALO)):
        halo[0, pl.ds(first, HALO)] = block[0:face, :].reshape(HALO, ny, nz)
        if columns:
            halo[1, pl.ds(first, HALO)] = unpacked(block[face : face + 2 * columns, :], columns, nz).reshape(HALO, ny, nz)
    for t in range(tiles):
        for x in range(nx):
            total = None
            for k, weight in enumerate(WEIGHTS, 1):
                for at in (x - k, x + k):
                    if 0 <= at < nx:
                        continue
                    term = jnp.float32(weight) * halo[t, at + HALO if at < 0 else at - nx + HALO]
                    total = term if total is None else total + term
            value = partial[t, x] if tiles == 2 else partial[x]
            if total is not None:
                value = value + rate[t, x] * total
            if tiles == 2:
                following[t, x] = value
            else:
                following[x] = value

    if tiles == 2:
        pack_faces(following, extra(step + 1), pair, y_low, y_high, rows)


def arrays(*shapes):
    return tuple(jax.ShapeDtypeStruct(s, jnp.float32) for s in shapes)


def face_shapes(shape, columns):
    nx, ny, nz = shape
    return (
        (2 * (HALO * ny + 2 * columns), nz),
        (HALO * nx + 2 * columns, nz),
        (HALO * nx + 2 * columns, nz),
    )


def call(kernel, out, inputs, operands, scratch=()):
    return pl.pallas_call(
        kernel,
        out_shape=out,
        in_specs=inputs,
        out_specs=(VMEM,) * len(out),
        scratch_shapes=[pltpu.VMEM(s, jnp.float32) for s in scratch],
        compiler_params=pltpu.CompilerParams(vmem_limit_bytes=16 * 1024 * 1024),
        cost_estimate=pl.CostEstimate(flops=5000000, bytes_accessed=1500000, transcendentals=0),
    )(*operands)


def line(count):
    return [(i, i + 1) for i in range(count - 1)]


def back(pairs):
    return [(b, a) for a, b in pairs]


def exchange(faces, ny, columns):
    pair, y_low, y_high = faces
    half = HALO * ny + 2 * columns
    count = lax.axis_size("gx")
    swapped = lax.ppermute(pair, "gx", [(i, i ^ 1) for i in range(count)])
    up = line(lax.axis_size("gy"))
    from_y_low = lax.ppermute(y_high, "gy", up)
    from_y_high = lax.ppermute(y_low, "gy", back(up))
    onward = [(i, (i + 2 - 4 * (i % 2)) % count) for i in range(count)]
    outer = lax.ppermute(swapped[half:], "gx", onward)
    return swapped[:half], outer, from_y_low, from_y_high


def per_device(pressure_now, pressure_before, region_code, velocity, wavelet, source_cell):
    shape = pressure_now.shape
    nx, ny, nz = shape
    field = (2,) + shape
    rows = (HALO * nx, nz)
    grid_y = ny * lax.axis_size("gy")
    grid_z = nz * lax.axis_size("gz")
    x = source_cell // (grid_y * grid_z) - lax.axis_index("gx") * nx
    y = source_cell // grid_z % grid_y - lax.axis_index("gy") * ny
    z = source_cell % grid_z - lax.axis_index("gz") * nz
    inside = (x >= 0) & (x < nx) & (y >= 0) & (y < ny) & (z >= -DEEP) & (z < nz + DEEP)
    place = jnp.where(z < 0, z + 2 * nz, z)
    cells = jnp.where(inside, (((place // nz) * nx + x) * ny + y) * nz + place % nz, -1)
    cells = jnp.broadcast_to(cells[:, None], (cells.shape[0], nz))
    amounts = [jnp.broadcast_to(wavelet[step][:, None], (wavelet.shape[1], nz)) for step in range(STEPS)]

    deep = (3 * DEEP, nx * ny)
    in_hbm = pl.BlockSpec(memory_space=pltpu.HBM)
    rate, z_low, z_high = pl.pallas_call(
        first_kernel,
        out_shape=arrays(shape, deep, deep),
        in_specs=[in_hbm] * 4,
        out_specs=(VMEM,) * 3,
        scratch_shapes=[
            pltpu.SMEM(velocity.shape, jnp.float32),
            pltpu.VMEM(shape, jnp.float32),
            pltpu.VMEM(shape, jnp.float32),
            pltpu.VMEM(shape, jnp.int32),
            pltpu.SemaphoreType.DMA((4,)),
        ],
        compiler_params=pltpu.CompilerParams(vmem_limit_bytes=16 * 1024 * 1024),
        cost_estimate=pl.CostEstimate(flops=5000000, bytes_accessed=1500000, transcendentals=0),
        name="first",
    )(*(pltpu.with_memory_space_constraint(a, pltpu.HBM) for a in (velocity, pressure_now, pressure_before, region_code)))
    up = line(lax.axis_size("gz"))
    from_low = lax.ppermute(z_high, "gz", up)
    from_high = lax.ppermute(z_low, "gz", back(up))
    from_low, from_high, cells, *amounts = lax.optimization_barrier((from_low, from_high, cells, *amounts))
    current, before, rate, *faces = call(
        widen_kernel,
        arrays(field, field, field, *face_shapes(shape, extra(0))),
        [VMEM] * 5,
        (pressure_now, pressure_before, rate, from_low, from_high),
        scratch=[rows],
    )
    for step in range(STEPS):
        last = step == STEPS - 1
        inner, outer, y_low, y_high = exchange(faces, ny, extra(step))
        out = call(
            lambda *refs, step=step: part_one(step, *refs),
            arrays(shape, shape) if last else arrays(field),
            [VMEM] * 7,
            (current, before, rate, cells, amounts[step], y_low, y_high),
            scratch=[(2, nx, ny + 16, nz)],
        )
        partial = out[0]
        following, *faces = call(
            lambda *refs, step=step: part_two(step, *refs),
            arrays(shape) if last else arrays(field, *face_shapes(shape, extra(step + 1))),
            [VMEM] * 4,
            (partial, rate, inner, outer),
            scratch=[(2, 2 * HALO, ny, nz)] if last else [(2, 2 * HALO, ny, nz), rows],
        )
        before, current = (out[1], following) if last else (current, following)
    return current, before


def solution(mesh):
    field = P("gx", "gy", "gz")
    return jax.shard_map(
        per_device,
        mesh=mesh,
        in_specs=(field, field, field, P(), P(), P()),
        out_specs=(field, field),
        check_vma=False,
    )
```

```python
import jax
import jax.numpy as jnp
from jax import lax
from jax.experimental import pallas as pl
from jax.experimental.pallas import tpu as pltpu
from jax.sharding import PartitionSpec as P


STEPS = 6
CENTRE = -205.0 / 72.0
WEIGHTS = (8.0 / 5.0, -1.0 / 5.0, 8.0 / 315.0, -1.0 / 560.0)
HALO = 4
DEEP = HALO * STEPS
VMEM = pl.BlockSpec(memory_space=pltpu.VMEM)


def extra(step):
    return DEEP - HALO * (step + 1)


def matmul(a, b, contract):
    return lax.dot_general(
        a, b, (contract, ((), ())), precision=lax.Precision.HIGHEST, preferred_element_type=jnp.float32
    )


def chosen(columns, nz):
    row = lax.broadcasted_iota(jnp.int32, (2 * columns, nz), 0)
    lane = lax.broadcasted_iota(jnp.int32, (2 * columns, nz), 1)
    wanted = jnp.where(row < columns, row, row + nz - 2 * columns)
    return jnp.where(lane == wanted, jnp.float32(1), jnp.float32(0))


def packed(rows, columns):
    return matmul(chosen(columns, rows.shape[1]), rows, ((1,), (1,)))


def unpacked(block, columns, nz):
    return matmul(block, chosen(columns, nz), ((0,), (0,)))


def pack_pair(field, columns, pair):
    _, nx, ny, nz = field.shape
    odd = lax.axis_index("gx") % 2
    inner = (1 - odd) * (nx - HALO)
    outer = odd * (nx - HALO)
    face = HALO * ny
    for place, first in ((0, inner), (face + 2 * columns, outer)):
        pair[place : place + face, :] = field[0, pl.ds(first, HALO)].reshape(face, nz)
        if columns:
            pair[place + face : place + face + 2 * columns, :] = packed(
                field[1, pl.ds(first, HALO)].reshape(face, nz), columns
            )


def pack_y(columns, field, y_low, y_high, rows):
    _, nx, ny, _ = field.shape
    for y_face, y in ((y_low, 0), (y_high, ny - HALO)):
        for x in range(nx):
            y_face[HALO * x : HALO * (x + 1), :] = field[0, x, y : y + HALO, :]
        if columns:
            for x in range(nx):
                rows[HALO * x : HALO * (x + 1), :] = field[1, x, y : y + HALO, :]
            y_face[HALO * nx : HALO * nx + 2 * columns, 0 : HALO * nx] = packed(rows[...], columns)


def first_kernel(velocity_in, now_in, before_in, codes_in, rate, z_low, z_high, velocity, now, before, codes, arrived):
    nx, ny, nz = now.shape
    regions = velocity.shape[0]
    copies = [
        pltpu.make_async_copy(source, target, arrived.at[n])
        for n, (source, target) in enumerate(
            ((velocity_in, velocity), (codes_in, codes), (now_in, now), (before_in, before))
        )
    ]
    for copy in copies:
        copy.start()
    copies[0].wait()
    copies[1].wait()
    squares = [velocity[r] * velocity[r] for r in range(regions)]
    for x in range(nx):
        code = codes[x]
        value = jnp.full(code.shape, squares[0], jnp.float32)
        for r in range(1, regions):
            value = jnp.where(code == r, squares[r], value)
        rate[x] = value
    copies[2].wait()
    copies[3].wait()
    for place, field in enumerate((now, before, rate)):
        both = packed(field[...].reshape(nx * ny, nz), DEEP)
        z_low[place * DEEP : (place + 1) * DEEP, :] = both[0:DEEP]
        z_high[place * DEEP : (place + 1) * DEEP, :] = both[DEEP : 2 * DEEP]


def widen(place, field, from_low, from_high, wide):
    nx, ny, nz = field.shape
    wide[0] = field[...]
    part = slice(place * DEEP, (place + 1) * DEEP)
    block = jnp.concatenate([from_high[part, :], from_low[part, :]], axis=0)
    wide[1] = unpacked(block, DEEP, nz).reshape(nx, ny, nz)


def widen_now(now, from_low, from_high, wide_now, pair):
    widen(0, now, from_low, from_high, wide_now)
    pack_pair(wide_now, extra(0), pair)


def widen_rest(before, rate, from_low, from_high, wide_before, wide_rate):
    widen(1, before, from_low, from_high, wide_before)
    widen(2, rate, from_low, from_high, wide_rate)


def part_one(step, now, before, rate, cells, amounts, y_low, y_high, *rest):
    following, wide = rest[0], rest[-1]
    columns = extra(step)
    tiles = 2 if columns else 1
    _, nx, ny, nz = now.shape
    for t in range(tiles):
        for place, y_face in ((8 - HALO, y_low), (8 + ny, y_high)):
            if t == 0:
                face = y_face[0 : HALO * nx, :]
            else:
                face = unpacked(y_face[HALO * nx : HALO * nx + 2 * columns, 0 : HALO * nx], columns, nz)
            for x in range(nx):
                wide[t, x, place : place + HALO, :] = face[HALO * x : HALO * (x + 1), :]
        for x in range(nx):
            wide[t, x, 8 : 8 + ny, :] = now[t, x]
    both = jnp.concatenate([now[0].reshape(nx * ny, nz), now[1].reshape(nx * ny, nz)], axis=1)
    i = lax.broadcasted_iota(jnp.int32, (2 * nz, tiles * nz), 0)
    j = lax.broadcasted_iota(jnp.int32, (2 * nz, tiles * nz), 1)
    distance = jnp.abs(i - j)
    distance = jnp.minimum(distance, 2 * nz - distance)
    band = jnp.zeros(distance.shape, jnp.float32)
    for k, weight in enumerate(WEIGHTS, 1):
        band = jnp.where(distance == k, jnp.float32(weight), band)
    along_z = matmul(both, band, ((1,), (0,)))
    for t in range(tiles):
        mine = along_z[:, t * nz : (t + 1) * nz].reshape(nx, ny, nz)
        for x in range(nx):
            here = now[t, x]
            total = jnp.float32(3.0 * CENTRE) * here + mine[x]
            for k, weight in enumerate(WEIGHTS, 1):
                around = wide[t, x, 8 + k : 8 + k + ny, :] + wide[t, x, 8 - k : 8 - k + ny, :]
                if x + k < nx:
                    around = around + now[t, x + k]
                if x - k >= 0:
                    around = around + now[t, x - k]
                total = total + jnp.float32(weight) * around
            value = 2.0 * here - before[t, x] + rate[t, x] * total
            if tiles == 2:
                following[t, x] = value
            else:
                following[x] = value
    if tiles == 1:
        rest[1][...] = now[0]

    @pl.when(jnp.max(cells[...]) >= 0)
    def _():
        lanes = lax.broadcasted_iota(jnp.int32, (1, nz), 1)
        numbers = [jnp.max(cells[s : s + 1, :]) for s in range(cells.shape[0])]
        for s, number in enumerate(numbers):

            @pl.when((number >= 0) & (number < tiles * nx * ny * nz))
            def _():
                line_of = number // nz
                y = line_of % ny
                x = line_of // ny % nx
                if tiles == 2:
                    here = following.at[line_of // (nx * ny), x]
                else:
                    here = following.at[x]
                row = here[pl.ds(y, 1), :]
                here[pl.ds(y, 1), :] = row + jnp.where(lanes == number % nz, amounts[s : s + 1, :], jnp.float32(0))


def part_two(step, partial, rate, inner, outer, following, *rest):
    columns = extra(step)
    tiles = 2 if columns else 1
    _, nx, ny, nz = rate.shape
    halo = rest[-1]
    odd = lax.axis_index("gx") % 2
    face = HALO * ny
    for block, first in ((inner, (1 - odd) * HALO), (outer, odd * HALO)):
        halo[0, pl.ds(first, HALO)] = block[0:face, :].reshape(HALO, ny, nz)
        if columns:
            halo[1, pl.ds(first, HALO)] = unpacked(block[face : face + 2 * columns, :], columns, nz).reshape(HALO, ny, nz)
    for t in range(tiles):
        for x in range(nx):
            total = None
            for k, weight in enumerate(WEIGHTS, 1):
                for at in (x - k, x + k):
                    if 0 <= at < nx:
                        continue
                    term = jnp.float32(weight) * halo[t, at + HALO if at < 0 else at - nx + HALO]
                    total = term if total is None else total + term
            value = partial[t, x] if tiles == 2 else partial[x]
            if total is not None:
                value = value + rate[t, x] * total
            if tiles == 2:
                following[t, x] = value
            else:
                following[x] = value

    if tiles == 2:
        pack_pair(following, extra(step + 1), rest[0])


def arrays(*shapes):
    return tuple(jax.ShapeDtypeStruct(s, jnp.float32) for s in shapes)


def pair_shape(shape, columns):
    _, ny, nz = shape
    return (2 * (HALO * ny + 2 * columns), nz)


def y_faces(field, columns):
    _, nx, _, nz = field.shape
    face = (HALO * nx + 2 * columns, nz)
    return call(lambda *refs: pack_y(columns, *refs), arrays(face, face), [VMEM], (field,), scratch=[(HALO * nx, nz)])


def call(kernel, out, inputs, operands, scratch=()):
    return pl.pallas_call(
        kernel,
        out_shape=out,
        in_specs=inputs,
        out_specs=(VMEM,) * len(out),
        scratch_shapes=[pltpu.VMEM(s, jnp.float32) for s in scratch],
        compiler_params=pltpu.CompilerParams(vmem_limit_bytes=16 * 1024 * 1024),
        cost_estimate=pl.CostEstimate(flops=5000000, bytes_accessed=1500000, transcendentals=0),
    )(*operands)


def line(count):
    return [(i, i + 1) for i in range(count - 1)]


def back(pairs):
    return [(b, a) for a, b in pairs]


def exchange(field, pair, columns):
    ny = field.shape[2]
    half = HALO * ny + 2 * columns
    count = lax.axis_size("gx")
    swapped = lax.ppermute(pair, "gx", [(i, i ^ 1) for i in range(count)])
    y_low, y_high = y_faces(field, columns)
    up = line(lax.axis_size("gy"))
    from_y_low = lax.ppermute(y_high, "gy", up)
    from_y_high = lax.ppermute(y_low, "gy", back(up))
    onward = [(i, (i + 2 - 4 * (i % 2)) % count) for i in range(count)]
    outer = lax.ppermute(swapped[half:], "gx", onward)
    return swapped[:half], outer, from_y_low, from_y_high


def per_device(pressure_now, pressure_before, region_code, velocity, wavelet, source_cell):
    shape = pressure_now.shape
    nx, ny, nz = shape
    field = (2,) + shape
    grid_y = ny * lax.axis_size("gy")
    grid_z = nz * lax.axis_size("gz")
    x = source_cell // (grid_y * grid_z) - lax.axis_index("gx") * nx
    y = source_cell // grid_z % grid_y - lax.axis_index("gy") * ny
    z = source_cell % grid_z - lax.axis_index("gz") * nz
    inside = (x >= 0) & (x < nx) & (y >= 0) & (y < ny) & (z >= -DEEP) & (z < nz + DEEP)
    place = jnp.where(z < 0, z + 2 * nz, z)
    cells = jnp.where(inside, (((place // nz) * nx + x) * ny + y) * nz + place % nz, -1)
    cells = jnp.broadcast_to(cells[:, None], (cells.shape[0], nz))
    amounts = [jnp.broadcast_to(wavelet[step][:, None], (wavelet.shape[1], nz)) for step in range(STEPS)]

    deep = (3 * DEEP, nx * ny)
    in_hbm = pl.BlockSpec(memory_space=pltpu.HBM)
    rate, z_low, z_high = pl.pallas_call(
        first_kernel,
        out_shape=arrays(shape, deep, deep),
        in_specs=[in_hbm] * 4,
        out_specs=(VMEM,) * 3,
        scratch_shapes=[
            pltpu.SMEM(velocity.shape, jnp.float32),
            pltpu.VMEM(shape, jnp.float32),
            pltpu.VMEM(shape, jnp.float32),
            pltpu.VMEM(shape, jnp.int32),
            pltpu.SemaphoreType.DMA((4,)),
        ],
        compiler_params=pltpu.CompilerParams(vmem_limit_bytes=16 * 1024 * 1024),
        cost_estimate=pl.CostEstimate(flops=5000000, bytes_accessed=1500000, transcendentals=0),
        name="first",
    )(*(pltpu.with_memory_space_constraint(a, pltpu.HBM) for a in (velocity, pressure_now, pressure_before, region_code)))
    up = line(lax.axis_size("gz"))
    from_low = lax.ppermute(z_high, "gz", up)
    from_high = lax.ppermute(z_low, "gz", back(up))
    from_low, from_high, cells, *amounts = lax.optimization_barrier((from_low, from_high, cells, *amounts))
    current, pair = call(
        widen_now, arrays(field, pair_shape(shape, extra(0))), [VMEM] * 3, (pressure_now, from_low, from_high)
    )
    before, rate = call(widen_rest, arrays(field, field), [VMEM] * 4, (pressure_before, rate, from_low, from_high))
    for step in range(STEPS):
        last = step == STEPS - 1
        inner, outer, y_low, y_high = exchange(current, pair, extra(step))
        out = call(
            lambda *refs, step=step: part_one(step, *refs),
            arrays(shape, shape) if last else arrays(field),
            [VMEM] * 7,
            (current, before, rate, cells, amounts[step], y_low, y_high),
            scratch=[(2, nx, ny + 16, nz)],
        )
        partial = out[0]
        following, *pairs = call(
            lambda *refs, step=step: part_two(step, *refs),
            arrays(shape) if last else arrays(field, pair_shape(shape, extra(step + 1))),
            [VMEM] * 4,
            (partial, rate, inner, outer),
            scratch=[(2, 2 * HALO, ny, nz)],
        )
        pair = pairs[0] if pairs else None
        before, current = (out[1], following) if last else (current, following)
    return current, before


def solution(mesh):
    field = P("gx", "gy", "gz")
    return jax.shard_map(
        per_device,
        mesh=mesh,
        in_specs=(field, field, field, P(), P(), P()),
        out_specs=(field, field),
        check_vma=False,
    )
```

```python
import jax
import jax.numpy as jnp
from jax import lax
from jax.experimental import pallas as pl
from jax.experimental.pallas import tpu as pltpu
from jax.sharding import PartitionSpec as P


STEPS = 6
CENTRE = -205.0 / 72.0
WEIGHTS = (8.0 / 5.0, -1.0 / 5.0, 8.0 / 315.0, -1.0 / 560.0)
HALO = 4
DEEP = HALO * STEPS
VMEM = pl.BlockSpec(memory_space=pltpu.VMEM)


def extra(step):
    return DEEP - HALO * (step + 1)


def matmul(a, b, contract):
    return lax.dot_general(
        a, b, (contract, ((), ())), precision=lax.Precision.HIGHEST, preferred_element_type=jnp.float32
    )


def chosen(columns, nz):
    row = lax.broadcasted_iota(jnp.int32, (2 * columns, nz), 0)
    lane = lax.broadcasted_iota(jnp.int32, (2 * columns, nz), 1)
    wanted = jnp.where(row < columns, row, row + nz - 2 * columns)
    return jnp.where(lane == wanted, jnp.float32(1), jnp.float32(0))


def packed(rows, columns):
    return matmul(chosen(columns, rows.shape[1]), rows, ((1,), (1,)))


def unpacked(block, columns, nz):
    return matmul(block, chosen(columns, nz), ((0,), (0,)))


def side(place):
    odd = lax.axis_index("gx") % 2
    return 1 - odd if place == "inner" else odd


def pack_x(field, columns, place, face_ref, first=0):
    _, nx, ny, nz = field.shape
    start = side(place) * (nx - HALO)
    face = HALO * ny
    face_ref[first : first + face, :] = field[0, pl.ds(start, HALO)].reshape(face, nz)
    if columns:
        face_ref[first + face : first + face + 2 * columns, :] = packed(
            field[1, pl.ds(start, HALO)].reshape(face, nz), columns
        )


def add_x(field, rate, columns, place, block, halo):
    _, nx, ny, nz = rate.shape
    face = HALO * ny
    high = side(place)
    tiles = 2 if columns else 1
    halo[0] = block[0:face, :].reshape(HALO, ny, nz)
    if columns:
        halo[1] = unpacked(block[face : face + 2 * columns, :], columns, nz).reshape(HALO, ny, nz)
    for t in range(tiles):
        beyond = [halo[t, high * (m - 1) + (1 - high) * (HALO - m)] for m in range(1, HALO + 1)]
        for j in range(HALO):
            x = high * (nx - 1 - j) + (1 - high) * j
            total = None
            for m in range(1, HALO + 1 - j):
                term = jnp.float32(WEIGHTS[j + m - 1]) * beyond[m - 1]
                total = term if total is None else total + term
            if len(field.shape) == 4:
                field[t, x] = field[t, x] + rate[t, x] * total
            else:
                field[x] = field[x] + rate[t, x] * total


def pack_y(columns, field, y_low, y_high, rows):
    _, nx, ny, _ = field.shape
    for y_face, y in ((y_low, 0), (y_high, ny - HALO)):
        for x in range(nx):
            y_face[HALO * x : HALO * (x + 1), :] = field[0, x, y : y + HALO, :]
        if columns:
            for x in range(nx):
                rows[HALO * x : HALO * (x + 1), :] = field[1, x, y : y + HALO, :]
            y_face[HALO * nx : HALO * nx + 2 * columns, 0 : HALO * nx] = packed(rows[...], columns)


def first_kernel(velocity_in, now_in, before_in, codes_in, rate, z_low, z_high, velocity, now, before, codes, arrived):
    nx, ny, nz = now.shape
    regions = velocity.shape[0]
    copies = [
        pltpu.make_async_copy(source, target, arrived.at[n])
        for n, (source, target) in enumerate(
            ((velocity_in, velocity), (codes_in, codes), (now_in, now), (before_in, before))
        )
    ]
    for copy in copies:
        copy.start()
    copies[0].wait()
    copies[1].wait()
    squares = [velocity[r] * velocity[r] for r in range(regions)]
    for x in range(nx):
        code = codes[x]
        value = jnp.full(code.shape, squares[0], jnp.float32)
        for r in range(1, regions):
            value = jnp.where(code == r, squares[r], value)
        rate[x] = value
    copies[2].wait()
    copies[3].wait()
    for place, field in enumerate((now, before, rate)):
        both = packed(field[...].reshape(nx * ny, nz), DEEP)
        z_low[place * DEEP : (place + 1) * DEEP, :] = both[0:DEEP]
        z_high[place * DEEP : (place + 1) * DEEP, :] = both[DEEP : 2 * DEEP]


def widen(place, field, from_low, from_high, wide):
    nx, ny, nz = field.shape
    wide[0] = field[...]
    part = slice(place * DEEP, (place + 1) * DEEP)
    block = jnp.concatenate([from_high[part, :], from_low[part, :]], axis=0)
    wide[1] = unpacked(block, DEEP, nz).reshape(nx, ny, nz)


def widen_now(now, from_low, from_high, wide_now, pair):
    widen(0, now, from_low, from_high, wide_now)
    pack_x(wide_now, extra(0), "inner", pair)
    pack_x(wide_now, extra(0), "outer", pair, pair.shape[0] // 2)


def widen_rest(before, rate, from_low, from_high, wide_before, wide_rate):
    widen(1, before, from_low, from_high, wide_before)
    widen(2, rate, from_low, from_high, wide_rate)


def part_one(step, now, before, rate, cells, amounts, inner, y_low, y_high, *rest):
    following, wide, halo = rest[0], rest[-2], rest[-1]
    columns = extra(step)
    tiles = 2 if columns else 1
    _, nx, ny, nz = now.shape
    for t in range(tiles):
        for place, y_face in ((8 - HALO, y_low), (8 + ny, y_high)):
            if t == 0:
                face = y_face[0 : HALO * nx, :]
            else:
                face = unpacked(y_face[HALO * nx : HALO * nx + 2 * columns, 0 : HALO * nx], columns, nz)
            for x in range(nx):
                wide[t, x, place : place + HALO, :] = face[HALO * x : HALO * (x + 1), :]
        for x in range(nx):
            wide[t, x, 8 : 8 + ny, :] = now[t, x]
    both = jnp.concatenate([now[0].reshape(nx * ny, nz), now[1].reshape(nx * ny, nz)], axis=1)
    i = lax.broadcasted_iota(jnp.int32, (2 * nz, tiles * nz), 0)
    j = lax.broadcasted_iota(jnp.int32, (2 * nz, tiles * nz), 1)
    distance = jnp.abs(i - j)
    distance = jnp.minimum(distance, 2 * nz - distance)
    band = jnp.zeros(distance.shape, jnp.float32)
    for k, weight in enumerate(WEIGHTS, 1):
        band = jnp.where(distance == k, jnp.float32(weight), band)
    along_z = matmul(both, band, ((1,), (0,)))
    for t in range(tiles):
        mine = along_z[:, t * nz : (t + 1) * nz].reshape(nx, ny, nz)
        for x in range(nx):
            here = now[t, x]
            total = jnp.float32(3.0 * CENTRE) * here + mine[x]
            for k, weight in enumerate(WEIGHTS, 1):
                around = wide[t, x, 8 + k : 8 + k + ny, :] + wide[t, x, 8 - k : 8 - k + ny, :]
                if x + k < nx:
                    around = around + now[t, x + k]
                if x - k >= 0:
                    around = around + now[t, x - k]
                total = total + jnp.float32(weight) * around
            value = 2.0 * here - before[t, x] + rate[t, x] * total
            if tiles == 2:
                following[t, x] = value
            else:
                following[x] = value
    if tiles == 1:
        rest[1][...] = now[0]
    add_x(following, rate, columns, "inner", inner, halo)

    @pl.when(jnp.max(cells[...]) >= 0)
    def _():
        lanes = lax.broadcasted_iota(jnp.int32, (1, nz), 1)
        numbers = [jnp.max(cells[s : s + 1, :]) for s in range(cells.shape[0])]
        for s, number in enumerate(numbers):

            @pl.when((number >= 0) & (number < tiles * nx * ny * nz))
            def _():
                line_of = number // nz
                y = line_of % ny
                x = line_of // ny % nx
                if tiles == 2:
                    here = following.at[line_of // (nx * ny), x]
                else:
                    here = following.at[x]
                row = here[pl.ds(y, 1), :]
                here[pl.ds(y, 1), :] = row + jnp.where(lanes == number % nz, amounts[s : s + 1, :], jnp.float32(0))
    if tiles == 2:
        pack_x(following, extra(step + 1), "inner", rest[1])


def part_two(step, partial, rate, outer, *rest):
    columns = extra(step)
    halo = rest[-1]
    following = rest[1] if columns else rest[0]
    following[...] = partial[...]
    add_x(following, rate, columns, "outer", outer, halo)
    if columns:
        inner_face, pair = rest[0], rest[2]
        half = pair.shape[0] // 2
        pair[0:half, :] = inner_face[...]
        pack_x(following, extra(step + 1), "outer", pair, half)


def arrays(*shapes):
    return tuple(jax.ShapeDtypeStruct(s, jnp.float32) for s in shapes)


def face_shape(shape, columns):
    _, ny, nz = shape
    return (HALO * ny + 2 * columns, nz)


def pair_shape(shape, columns):
    rows, nz = face_shape(shape, columns)
    return (2 * rows, nz)


def y_faces(field, columns):
    _, nx, _, nz = field.shape
    face = (HALO * nx + 2 * columns, nz)
    return call(lambda *refs: pack_y(columns, *refs), arrays(face, face), [VMEM], (field,), scratch=[(HALO * nx, nz)])


def call(kernel, out, inputs, operands, scratch=()):
    return pl.pallas_call(
        kernel,
        out_shape=out,
        in_specs=inputs,
        out_specs=(VMEM,) * len(out),
        scratch_shapes=[pltpu.VMEM(s, jnp.float32) for s in scratch],
        compiler_params=pltpu.CompilerParams(vmem_limit_bytes=16 * 1024 * 1024),
        cost_estimate=pl.CostEstimate(flops=5000000, bytes_accessed=1500000, transcendentals=0),
    )(*operands)


def line(count):
    return [(i, i + 1) for i in range(count - 1)]


def back(pairs):
    return [(b, a) for a, b in pairs]


def exchange(field, pair, columns):
    ny = field.shape[2]
    half = HALO * ny + 2 * columns
    count = lax.axis_size("gx")
    swapped = lax.ppermute(pair, "gx", [(i, i ^ 1) for i in range(count)])
    y_low, y_high = y_faces(field, columns)
    up = line(lax.axis_size("gy"))
    from_y_low = lax.ppermute(y_high, "gy", up)
    from_y_high = lax.ppermute(y_low, "gy", back(up))
    onward = [(i, (i + 2 - 4 * (i % 2)) % count) for i in range(count)]
    outer = lax.ppermute(swapped[half:], "gx", onward)
    return swapped[:half], outer, from_y_low, from_y_high


def per_device(pressure_now, pressure_before, region_code, velocity, wavelet, source_cell):
    shape = pressure_now.shape
    nx, ny, nz = shape
    field = (2,) + shape
    grid_y = ny * lax.axis_size("gy")
    grid_z = nz * lax.axis_size("gz")
    x = source_cell // (grid_y * grid_z) - lax.axis_index("gx") * nx
    y = source_cell // grid_z % grid_y - lax.axis_index("gy") * ny
    z = source_cell % grid_z - lax.axis_index("gz") * nz
    inside = (x >= 0) & (x < nx) & (y >= 0) & (y < ny) & (z >= -DEEP) & (z < nz + DEEP)
    place = jnp.where(z < 0, z + 2 * nz, z)
    cells = jnp.where(inside, (((place // nz) * nx + x) * ny + y) * nz + place % nz, -1)
    cells = jnp.broadcast_to(cells[:, None], (cells.shape[0], nz))
    amounts = [jnp.broadcast_to(wavelet[step][:, None], (wavelet.shape[1], nz)) for step in range(STEPS)]

    deep = (3 * DEEP, nx * ny)
    in_hbm = pl.BlockSpec(memory_space=pltpu.HBM)
    rate, z_low, z_high = pl.pallas_call(
        first_kernel,
        out_shape=arrays(shape, deep, deep),
        in_specs=[in_hbm] * 4,
        out_specs=(VMEM,) * 3,
        scratch_shapes=[
            pltpu.SMEM(velocity.shape, jnp.float32),
            pltpu.VMEM(shape, jnp.float32),
            pltpu.VMEM(shape, jnp.float32),
            pltpu.VMEM(shape, jnp.int32),
            pltpu.SemaphoreType.DMA((4,)),
        ],
        compiler_params=pltpu.CompilerParams(vmem_limit_bytes=16 * 1024 * 1024),
        cost_estimate=pl.CostEstimate(flops=5000000, bytes_accessed=1500000, transcendentals=0),
        name="first",
    )(*(pltpu.with_memory_space_constraint(a, pltpu.HBM) for a in (velocity, pressure_now, pressure_before, region_code)))
    up = line(lax.axis_size("gz"))
    from_low = lax.ppermute(z_high, "gz", up)
    from_high = lax.ppermute(z_low, "gz", back(up))
    current, pair = call(
        widen_now, arrays(field, pair_shape(shape, extra(0))), [VMEM] * 3, (pressure_now, from_low, from_high)
    )
    before, rate = call(widen_rest, arrays(field, field), [VMEM] * 4, (pressure_before, rate, from_low, from_high))
    for step in range(STEPS):
        last = step == STEPS - 1
        inner, outer, y_low, y_high = exchange(current, pair, extra(step))
        out = call(
            lambda *refs, step=step: part_one(step, *refs),
            arrays(shape, shape) if last else arrays(field, face_shape(shape, extra(step + 1))),
            [VMEM] * 8,
            (current, before, rate, cells, amounts[step], inner, y_low, y_high),
            scratch=[(2, nx, ny + 16, nz), (2, HALO, ny, nz)],
        )
        partial = out[0]
        following, *pairs = call(
            lambda *refs, step=step: part_two(step, *refs),
            arrays(shape) if last else arrays(field, pair_shape(shape, extra(step + 1))),
            [VMEM] * (3 if last else 4),
            (partial, rate, outer) if last else (partial, rate, outer, out[1]),
            scratch=[(2, HALO, ny, nz)],
        )
        pair = pairs[0] if pairs else None
        before, current = (out[1], following) if last else (current, following)
    return current, before


def solution(mesh):
    field = P("gx", "gy", "gz")
    return jax.shard_map(
        per_device,
        mesh=mesh,
        in_specs=(field, field, field, P(), P(), P()),
        out_specs=(field, field),
        check_vma=False,
    )
```

```python
import jax
import jax.numpy as jnp
from jax import lax
from jax.experimental import pallas as pl
from jax.experimental.pallas import tpu as pltpu
from jax.sharding import PartitionSpec as P


STEPS = 6
CENTRE = -205.0 / 72.0
WEIGHTS = (8.0 / 5.0, -1.0 / 5.0, 8.0 / 315.0, -1.0 / 560.0)
HALO = 4
DEEP = HALO * STEPS
VMEM = pl.BlockSpec(memory_space=pltpu.VMEM)


def extra(step):
    return DEEP - HALO * (step + 1)


def matmul(a, b, contract):
    return lax.dot_general(
        a, b, (contract, ((), ())), precision=lax.Precision.HIGHEST, preferred_element_type=jnp.float32
    )


def chosen(columns, nz):
    row = lax.broadcasted_iota(jnp.int32, (2 * columns, nz), 0)
    lane = lax.broadcasted_iota(jnp.int32, (2 * columns, nz), 1)
    wanted = jnp.where(row < columns, row, row + nz - 2 * columns)
    return jnp.where(lane == wanted, jnp.float32(1), jnp.float32(0))


def packed(rows, columns):
    return matmul(chosen(columns, rows.shape[1]), rows, ((1,), (1,)))


def unpacked(block, columns, nz):
    return matmul(block, chosen(columns, nz), ((0,), (0,)))


def side(place):
    odd = lax.axis_index("gx") % 2
    return 1 - odd if place == "inner" else odd


def pack_x(field, columns, place, face_ref, first=0):
    _, nx, ny, nz = field.shape
    start = side(place) * (nx - HALO)
    face = HALO * ny
    face_ref[first : first + face, :] = field[0, pl.ds(start, HALO)].reshape(face, nz)
    if columns:
        face_ref[first + face : first + face + 2 * columns, :] = packed(
            field[1, pl.ds(start, HALO)].reshape(face, nz), columns
        )


def add_x(field, rate, columns, place, block, halo):
    _, nx, ny, nz = rate.shape
    face = HALO * ny
    high = side(place)
    tiles = 2 if columns else 1
    halo[0] = block[0:face, :].reshape(HALO, ny, nz)
    if columns:
        halo[1] = unpacked(block[face : face + 2 * columns, :], columns, nz).reshape(HALO, ny, nz)
    for t in range(tiles):
        beyond = [halo[t, high * (m - 1) + (1 - high) * (HALO - m)] for m in range(1, HALO + 1)]
        for j in range(HALO):
            x = high * (nx - 1 - j) + (1 - high) * j
            total = None
            for m in range(1, HALO + 1 - j):
                term = jnp.float32(WEIGHTS[j + m - 1]) * beyond[m - 1]
                total = term if total is None else total + term
            if len(field.shape) == 4:
                field[t, x] = field[t, x] + rate[t, x] * total
            else:
                field[x] = field[x] + rate[t, x] * total


def pack_y(columns, field, y_low, y_high, rows):
    _, nx, ny, _ = field.shape
    for y_face, y in ((y_low, 0), (y_high, ny - HALO)):
        for x in range(nx):
            y_face[HALO * x : HALO * (x + 1), :] = field[0, x, y : y + HALO, :]
        if columns:
            for x in range(nx):
                rows[HALO * x : HALO * (x + 1), :] = field[1, x, y : y + HALO, :]
            y_face[HALO * nx : HALO * nx + 2 * columns, 0 : HALO * nx] = packed(rows[...], columns)


def first_kernel(velocity_in, now_in, before_in, codes_in, rate, z_low, z_high, velocity, now, before, codes, arrived):
    nx, ny, nz = now.shape
    regions = velocity.shape[0]
    copies = [
        pltpu.make_async_copy(source, target, arrived.at[n])
        for n, (source, target) in enumerate(
            ((velocity_in, velocity), (codes_in, codes), (now_in, now), (before_in, before))
        )
    ]
    for copy in copies:
        copy.start()
    copies[0].wait()
    copies[1].wait()
    squares = [velocity[r] * velocity[r] for r in range(regions)]
    for x in range(nx):
        code = codes[x]
        value = jnp.full(code.shape, squares[0], jnp.float32)
        for r in range(1, regions):
            value = jnp.where(code == r, squares[r], value)
        rate[x] = value
    copies[2].wait()
    copies[3].wait()
    for place, field in enumerate((now, before, rate)):
        both = packed(field[...].reshape(nx * ny, nz), DEEP)
        z_low[place * DEEP : (place + 1) * DEEP, :] = both[0:DEEP]
        z_high[place * DEEP : (place + 1) * DEEP, :] = both[DEEP : 2 * DEEP]


def widen(place, field, from_low, from_high, wide):
    nx, ny, nz = field.shape
    wide[0] = field[...]
    part = slice(place * DEEP, (place + 1) * DEEP)
    block = jnp.concatenate([from_high[part, :], from_low[part, :]], axis=0)
    wide[1] = unpacked(block, DEEP, nz).reshape(nx, ny, nz)


def widen_now(now, from_low, from_high, wide_now, pair):
    widen(0, now, from_low, from_high, wide_now)
    pack_x(wide_now, extra(0), "inner", pair)
    pack_x(wide_now, extra(0), "outer", pair, pair.shape[0] // 2)


def widen_rest(before, rate, from_low, from_high, wide_before, wide_rate):
    widen(1, before, from_low, from_high, wide_before)
    widen(2, rate, from_low, from_high, wide_rate)


def part_zero(step, now, before, rate, *rest):
    following, wide = rest[0], rest[-1]
    columns = extra(step)
    tiles = 2 if columns else 1
    _, nx, ny, nz = now.shape
    edge = jnp.zeros((HALO, nz), jnp.float32)
    for t in range(tiles):
        for x in range(nx):
            wide[t, x, 8 - HALO : 8, :] = edge
            wide[t, x, 8 : 8 + ny, :] = now[t, x]
            wide[t, x, 8 + ny : 8 + ny + HALO, :] = edge
    both = jnp.concatenate([now[0].reshape(nx * ny, nz), now[1].reshape(nx * ny, nz)], axis=1)
    i = lax.broadcasted_iota(jnp.int32, (2 * nz, tiles * nz), 0)
    j = lax.broadcasted_iota(jnp.int32, (2 * nz, tiles * nz), 1)
    distance = jnp.abs(i - j)
    distance = jnp.minimum(distance, 2 * nz - distance)
    band = jnp.zeros(distance.shape, jnp.float32)
    for k, weight in enumerate(WEIGHTS, 1):
        band = jnp.where(distance == k, jnp.float32(weight), band)
    along_z = matmul(both, band, ((1,), (0,)))
    for t in range(tiles):
        mine = along_z[:, t * nz : (t + 1) * nz].reshape(nx, ny, nz)
        for x in range(nx):
            here = now[t, x]
            total = jnp.float32(3.0 * CENTRE) * here + mine[x]
            for k, weight in enumerate(WEIGHTS, 1):
                around = wide[t, x, 8 + k : 8 + k + ny, :] + wide[t, x, 8 - k : 8 - k + ny, :]
                if x + k < nx:
                    around = around + now[t, x + k]
                if x - k >= 0:
                    around = around + now[t, x - k]
                total = total + jnp.float32(weight) * around
            value = 2.0 * here - before[t, x] + rate[t, x] * total
            if tiles == 2:
                following[t, x] = value
            else:
                following[x] = value
    if tiles == 1:
        rest[1][...] = now[0]


def part_one(step, partial, rate, cells, amounts, inner, y_low, y_high, *rest):
    following, halo, beside = rest[0], rest[-2], rest[-1]
    columns = extra(step)
    tiles = 2 if columns else 1
    _, nx, ny, nz = rate.shape
    zeros = jnp.zeros((8, nz), jnp.float32)
    for t in range(tiles):
        for x in range(nx):
            beside[0, t, x, 8:16, :] = zeros
            beside[1, t, x, 0:8, :] = zeros
        for n, (y_face, first) in enumerate(((y_low, 4), (y_high, 8))):
            if t == 0:
                face = y_face[0 : HALO * nx, :]
            else:
                face = unpacked(y_face[HALO * nx : HALO * nx + 2 * columns, 0 : HALO * nx], columns, nz)
            for x in range(nx):
                beside[n, t, x, first : first + HALO, :] = face[HALO * x : HALO * (x + 1), :]
        for x in range(nx):
            low = high = None
            for k, weight in enumerate(WEIGHTS, 1):
                term = jnp.float32(weight) * beside[0, t, x, 8 - k : 16 - k, :]
                low = term if low is None else low + term
                term = jnp.float32(weight) * beside[1, t, x, k : 8 + k, :]
                high = term if high is None else high + term
            old = partial.at[t, x] if tiles == 2 else partial.at[x]
            new = following.at[t, x] if tiles == 2 else following.at[x]
            new[0:8, :] = old[0:8, :] + rate[t, x, 0:8, :] * low
            new[8 : ny - 8, :] = old[8 : ny - 8, :]
            new[ny - 8 : ny, :] = old[ny - 8 : ny, :] + rate[t, x, ny - 8 : ny, :] * high
    add_x(following, rate, columns, "inner", inner, halo)

    @pl.when(jnp.max(cells[...]) >= 0)
    def _():
        lanes = lax.broadcasted_iota(jnp.int32, (1, nz), 1)
        numbers = [jnp.max(cells[s : s + 1, :]) for s in range(cells.shape[0])]
        for s, number in enumerate(numbers):

            @pl.when((number >= 0) & (number < tiles * nx * ny * nz))
            def _():
                line_of = number // nz
                y = line_of % ny
                x = line_of // ny % nx
                if tiles == 2:
                    here = following.at[line_of // (nx * ny), x]
                else:
                    here = following.at[x]
                row = here[pl.ds(y, 1), :]
                here[pl.ds(y, 1), :] = row + jnp.where(lanes == number % nz, amounts[s : s + 1, :], jnp.float32(0))
    if tiles == 2:
        pack_x(following, extra(step + 1), "inner", rest[1])


def part_two(step, partial, rate, outer, *rest):
    columns = extra(step)
    halo = rest[-1]
    following = rest[1] if columns else rest[0]
    following[...] = partial[...]
    add_x(following, rate, columns, "outer", outer, halo)
    if columns:
        inner_face, pair = rest[0], rest[2]
        half = pair.shape[0] // 2
        pair[0:half, :] = inner_face[...]
        pack_x(following, extra(step + 1), "outer", pair, half)


def arrays(*shapes):
    return tuple(jax.ShapeDtypeStruct(s, jnp.float32) for s in shapes)


def face_shape(shape, columns):
    _, ny, nz = shape
    return (HALO * ny + 2 * columns, nz)


def pair_shape(shape, columns):
    rows, nz = face_shape(shape, columns)
    return (2 * rows, nz)


def y_faces(field, columns):
    _, nx, _, nz = field.shape
    face = (HALO * nx + 2 * columns, nz)
    return call(lambda *refs: pack_y(columns, *refs), arrays(face, face), [VMEM], (field,), scratch=[(HALO * nx, nz)])


def call(kernel, out, inputs, operands, scratch=()):
    return pl.pallas_call(
        kernel,
        out_shape=out,
        in_specs=inputs,
        out_specs=(VMEM,) * len(out),
        scratch_shapes=[pltpu.VMEM(s, jnp.float32) for s in scratch],
        compiler_params=pltpu.CompilerParams(vmem_limit_bytes=16 * 1024 * 1024),
        cost_estimate=pl.CostEstimate(flops=5000000, bytes_accessed=1500000, transcendentals=0),
    )(*operands)


def line(count):
    return [(i, i + 1) for i in range(count - 1)]


def back(pairs):
    return [(b, a) for a, b in pairs]


def exchange(field, pair, columns):
    ny = field.shape[2]
    half = HALO * ny + 2 * columns
    count = lax.axis_size("gx")
    swapped = lax.ppermute(pair, "gx", [(i, i ^ 1) for i in range(count)])
    y_low, y_high = y_faces(field, columns)
    up = line(lax.axis_size("gy"))
    from_y_low = lax.ppermute(y_high, "gy", up)
    from_y_high = lax.ppermute(y_low, "gy", back(up))
    onward = [(i, (i + 2 - 4 * (i % 2)) % count) for i in range(count)]
    outer = lax.ppermute(swapped[half:], "gx", onward)
    return swapped[:half], outer, from_y_low, from_y_high


def per_device(pressure_now, pressure_before, region_code, velocity, wavelet, source_cell):
    shape = pressure_now.shape
    nx, ny, nz = shape
    field = (2,) + shape
    grid_y = ny * lax.axis_size("gy")
    grid_z = nz * lax.axis_size("gz")
    x = source_cell // (grid_y * grid_z) - lax.axis_index("gx") * nx
    y = source_cell // grid_z % grid_y - lax.axis_index("gy") * ny
    z = source_cell % grid_z - lax.axis_index("gz") * nz
    inside = (x >= 0) & (x < nx) & (y >= 0) & (y < ny) & (z >= -DEEP) & (z < nz + DEEP)
    place = jnp.where(z < 0, z + 2 * nz, z)
    cells = jnp.where(inside, (((place // nz) * nx + x) * ny + y) * nz + place % nz, -1)
    cells = jnp.broadcast_to(cells[:, None], (cells.shape[0], nz))
    amounts = [jnp.broadcast_to(wavelet[step][:, None], (wavelet.shape[1], nz)) for step in range(STEPS)]

    deep = (3 * DEEP, nx * ny)
    in_hbm = pl.BlockSpec(memory_space=pltpu.HBM)
    rate, z_low, z_high = pl.pallas_call(
        first_kernel,
        out_shape=arrays(shape, deep, deep),
        in_specs=[in_hbm] * 4,
        out_specs=(VMEM,) * 3,
        scratch_shapes=[
            pltpu.SMEM(velocity.shape, jnp.float32),
            pltpu.VMEM(shape, jnp.float32),
            pltpu.VMEM(shape, jnp.float32),
            pltpu.VMEM(shape, jnp.int32),
            pltpu.SemaphoreType.DMA((4,)),
        ],
        compiler_params=pltpu.CompilerParams(vmem_limit_bytes=16 * 1024 * 1024),
        cost_estimate=pl.CostEstimate(flops=5000000, bytes_accessed=1500000, transcendentals=0),
        name="first",
    )(*(pltpu.with_memory_space_constraint(a, pltpu.HBM) for a in (velocity, pressure_now, pressure_before, region_code)))
    up = line(lax.axis_size("gz"))
    from_low = lax.ppermute(z_high, "gz", up)
    from_high = lax.ppermute(z_low, "gz", back(up))
    current, pair = call(
        widen_now, arrays(field, pair_shape(shape, extra(0))), [VMEM] * 3, (pressure_now, from_low, from_high)
    )
    before, rate = call(widen_rest, arrays(field, field), [VMEM] * 4, (pressure_before, rate, from_low, from_high))
    for step in range(STEPS):
        last = step == STEPS - 1
        inner, outer, y_low, y_high = exchange(current, pair, extra(step))
        early = call(
            lambda *refs, step=step: part_zero(step, *refs),
            arrays(shape, shape) if last else arrays(field),
            [VMEM] * 3,
            (current, before, rate),
            scratch=[(2, nx, ny + 16, nz)],
        )
        out = call(
            lambda *refs, step=step: part_one(step, *refs),
            arrays(shape) if last else arrays(field, face_shape(shape, extra(step + 1))),
            [VMEM] * 7,
            (early[0], rate, cells, amounts[step], inner, y_low, y_high),
            scratch=[(2, HALO, ny, nz), (2, 2, nx, 16, nz)],
        )
        partial = out[0]
        following, *pairs = call(
            lambda *refs, step=step: part_two(step, *refs),
            arrays(shape) if last else arrays(field, pair_shape(shape, extra(step + 1))),
            [VMEM] * (3 if last else 4),
            (partial, rate, outer) if last else (partial, rate, outer, out[1]),
            scratch=[(2, HALO, ny, nz)],
        )
        pair = pairs[0] if pairs else None
        before, current = (early[1], following) if last else (current, following)
    return current, before


def solution(mesh):
    field = P("gx", "gy", "gz")
    return jax.shard_map(
        per_device,
        mesh=mesh,
        in_specs=(field, field, field, P(), P(), P()),
        out_specs=(field, field),
        check_vma=False,
    )
```

```python
import jax
import jax.numpy as jnp
from jax import lax
from jax.experimental import pallas as pl
from jax.experimental.pallas import tpu as pltpu
from jax.sharding import PartitionSpec as P


STEPS = 6
CENTRE = -205.0 / 72.0
WEIGHTS = (8.0 / 5.0, -1.0 / 5.0, 8.0 / 315.0, -1.0 / 560.0)
HALO = 4
DEEP = HALO * STEPS
VMEM = pl.BlockSpec(memory_space=pltpu.VMEM)


def extra(step):
    return DEEP - HALO * (step + 1)


def matmul(a, b, contract):
    return lax.dot_general(
        a, b, (contract, ((), ())), precision=lax.Precision.HIGHEST, preferred_element_type=jnp.float32
    )


def chosen(columns, nz):
    row = lax.broadcasted_iota(jnp.int32, (2 * columns, nz), 0)
    lane = lax.broadcasted_iota(jnp.int32, (2 * columns, nz), 1)
    wanted = jnp.where(row < columns, row, row + nz - 2 * columns)
    return jnp.where(lane == wanted, jnp.float32(1), jnp.float32(0))


def packed(rows, columns):
    return matmul(chosen(columns, rows.shape[1]), rows, ((1,), (1,)))


def unpacked(block, columns, nz):
    return matmul(block, chosen(columns, nz), ((0,), (0,)))


def side(place):
    odd = lax.axis_index("gx") % 2
    return 1 - odd if place == "inner" else odd


def pack_x(field, columns, place, face_ref, first=0):
    _, nx, ny, nz = field.shape
    start = side(place) * (nx - HALO)
    face = HALO * ny
    face_ref[first : first + face, :] = field[0, pl.ds(start, HALO)].reshape(face, nz)
    if columns:
        face_ref[first + face : first + face + 2 * columns, :] = packed(
            field[1, pl.ds(start, HALO)].reshape(face, nz), columns
        )


def add_x(field, rate, columns, place, block, halo):
    _, nx, ny, nz = rate.shape
    face = HALO * ny
    high = side(place)
    tiles = 2 if columns else 1
    halo[0] = block[0:face, :].reshape(HALO, ny, nz)
    if columns:
        halo[1] = unpacked(block[face : face + 2 * columns, :], columns, nz).reshape(HALO, ny, nz)
    for t in range(tiles):
        beyond = [halo[t, high * (m - 1) + (1 - high) * (HALO - m)] for m in range(1, HALO + 1)]
        for j in range(HALO):
            x = high * (nx - 1 - j) + (1 - high) * j
            total = None
            for m in range(1, HALO + 1 - j):
                term = jnp.float32(WEIGHTS[j + m - 1]) * beyond[m - 1]
                total = term if total is None else total + term
            if len(field.shape) == 4:
                field[t, x] = field[t, x] + rate[t, x] * total
            else:
                field[x] = field[x] + rate[t, x] * total


def pack_y(columns, field, y_low, y_high, rows):
    _, nx, ny, _ = field.shape
    for y_face, y in ((y_low, 0), (y_high, ny - HALO)):
        for x in range(nx):
            y_face[HALO * x : HALO * (x + 1), :] = field[0, x, y : y + HALO, :]
        if columns:
            for x in range(nx):
                rows[HALO * x : HALO * (x + 1), :] = field[1, x, y : y + HALO, :]
            y_face[HALO * nx : HALO * nx + 2 * columns, 0 : HALO * nx] = packed(rows[...], columns)


def first_kernel(velocity_in, now_in, before_in, codes_in, rate, z_low, z_high, velocity, now, before, codes, arrived):
    nx, ny, nz = now.shape
    regions = velocity.shape[0]
    copies = [
        pltpu.make_async_copy(source, target, arrived.at[n])
        for n, (source, target) in enumerate(
            ((now_in, now), (before_in, before), (velocity_in, velocity), (codes_in, codes))
        )
    ]
    for copy in copies:
        copy.start()

    def pack(place, field):
        both = packed(field[...].reshape(nx * ny, nz), DEEP)
        z_low[place * DEEP : (place + 1) * DEEP, :] = both[0:DEEP]
        z_high[place * DEEP : (place + 1) * DEEP, :] = both[DEEP : 2 * DEEP]

    copies[0].wait()
    pack(0, now)
    copies[1].wait()
    pack(1, before)
    copies[2].wait()
    copies[3].wait()
    squares = [velocity[r] * velocity[r] for r in range(regions)]
    for x in range(nx):
        code = codes[x]
        value = jnp.full(code.shape, squares[0], jnp.float32)
        for r in range(1, regions):
            value = jnp.where(code == r, squares[r], value)
        rate[x] = value
    pack(2, rate)


def widen(place, field, from_low, from_high, wide):
    nx, ny, nz = field.shape
    wide[0] = field[...]
    part = slice(place * DEEP, (place + 1) * DEEP)
    block = jnp.concatenate([from_high[part, :], from_low[part, :]], axis=0)
    wide[1] = unpacked(block, DEEP, nz).reshape(nx, ny, nz)


def widen_now(now, from_low, from_high, wide_now, pair):
    widen(0, now, from_low, from_high, wide_now)
    pack_x(wide_now, extra(0), "inner", pair)
    pack_x(wide_now, extra(0), "outer", pair, pair.shape[0] // 2)


def widen_rest(before, rate, from_low, from_high, wide_before, wide_rate):
    widen(1, before, from_low, from_high, wide_before)
    widen(2, rate, from_low, from_high, wide_rate)


def part_zero(step, now, before, rate, *rest):
    following, wide = rest[0], rest[-1]
    columns = extra(step)
    tiles = 2 if columns else 1
    _, nx, ny, nz = now.shape
    edge = jnp.zeros((HALO, nz), jnp.float32)
    for t in range(tiles):
        for x in range(nx):
            wide[t, x, 8 - HALO : 8, :] = edge
            wide[t, x, 8 : 8 + ny, :] = now[t, x]
            wide[t, x, 8 + ny : 8 + ny + HALO, :] = edge
    both = jnp.concatenate([now[0].reshape(nx * ny, nz), now[1].reshape(nx * ny, nz)], axis=1)
    i = lax.broadcasted_iota(jnp.int32, (2 * nz, tiles * nz), 0)
    j = lax.broadcasted_iota(jnp.int32, (2 * nz, tiles * nz), 1)
    distance = jnp.abs(i - j)
    distance = jnp.minimum(distance, 2 * nz - distance)
    band = jnp.zeros(distance.shape, jnp.float32)
    for k, weight in enumerate(WEIGHTS, 1):
        band = jnp.where(distance == k, jnp.float32(weight), band)
    along_z = matmul(both, band, ((1,), (0,)))
    for t in range(tiles):
        mine = along_z[:, t * nz : (t + 1) * nz].reshape(nx, ny, nz)
        for x in range(nx):
            here = now[t, x]
            total = jnp.float32(3.0 * CENTRE) * here + mine[x]
            for k, weight in enumerate(WEIGHTS, 1):
                around = wide[t, x, 8 + k : 8 + k + ny, :] + wide[t, x, 8 - k : 8 - k + ny, :]
                if x + k < nx:
                    around = around + now[t, x + k]
                if x - k >= 0:
                    around = around + now[t, x - k]
                total = total + jnp.float32(weight) * around
            value = 2.0 * here - before[t, x] + rate[t, x] * total
            if tiles == 2:
                following[t, x] = value
            else:
                following[x] = value
    if tiles == 1:
        rest[1][...] = now[0]


def part_one(step, partial, rate, cells, amounts, inner, y_low, y_high, *rest):
    following, halo, beside = rest[0], rest[-2], rest[-1]
    columns = extra(step)
    tiles = 2 if columns else 1
    _, nx, ny, nz = rate.shape
    zeros = jnp.zeros((8, nz), jnp.float32)
    for t in range(tiles):
        for x in range(nx):
            beside[0, t, x, 8:16, :] = zeros
            beside[1, t, x, 0:8, :] = zeros
        for n, (y_face, first) in enumerate(((y_low, 4), (y_high, 8))):
            if t == 0:
                face = y_face[0 : HALO * nx, :]
            else:
                face = unpacked(y_face[HALO * nx : HALO * nx + 2 * columns, 0 : HALO * nx], columns, nz)
            for x in range(nx):
                beside[n, t, x, first : first + HALO, :] = face[HALO * x : HALO * (x + 1), :]
        for x in range(nx):
            low = high = None
            for k, weight in enumerate(WEIGHTS, 1):
                term = jnp.float32(weight) * beside[0, t, x, 8 - k : 16 - k, :]
                low = term if low is None else low + term
                term = jnp.float32(weight) * beside[1, t, x, k : 8 + k, :]
                high = term if high is None else high + term
            old = partial.at[t, x] if tiles == 2 else partial.at[x]
            new = following.at[t, x] if tiles == 2 else following.at[x]
            new[0:8, :] = old[0:8, :] + rate[t, x, 0:8, :] * low
            new[8 : ny - 8, :] = old[8 : ny - 8, :]
            new[ny - 8 : ny, :] = old[ny - 8 : ny, :] + rate[t, x, ny - 8 : ny, :] * high
    add_x(following, rate, columns, "inner", inner, halo)

    @pl.when(jnp.max(cells[...]) >= 0)
    def _():
        lanes = lax.broadcasted_iota(jnp.int32, (1, nz), 1)
        numbers = [jnp.max(cells[s : s + 1, :]) for s in range(cells.shape[0])]
        for s, number in enumerate(numbers):

            @pl.when((number >= 0) & (number < tiles * nx * ny * nz))
            def _():
                line_of = number // nz
                y = line_of % ny
                x = line_of // ny % nx
                if tiles == 2:
                    here = following.at[line_of // (nx * ny), x]
                else:
                    here = following.at[x]
                row = here[pl.ds(y, 1), :]
                here[pl.ds(y, 1), :] = row + jnp.where(lanes == number % nz, amounts[s : s + 1, :], jnp.float32(0))

    if tiles == 2:
        pack_x(following, extra(step + 1), "inner", rest[1])


def part_two(step, partial, rate, outer, *rest):
    columns = extra(step)
    halo = rest[-1]
    following = rest[1] if columns else rest[0]
    following[...] = partial[...]
    add_x(following, rate, columns, "outer", outer, halo)
    if columns:
        inner_face, pair = rest[0], rest[2]
        half = pair.shape[0] // 2
        pair[0:half, :] = inner_face[...]
        pack_x(following, extra(step + 1), "outer", pair, half)


def arrays(*shapes):
    return tuple(jax.ShapeDtypeStruct(s, jnp.float32) for s in shapes)


def face_shape(shape, columns):
    _, ny, nz = shape
    return (HALO * ny + 2 * columns, nz)


def pair_shape(shape, columns):
    rows, nz = face_shape(shape, columns)
    return (2 * rows, nz)


def y_faces(field, columns):
    _, nx, _, nz = field.shape
    face = (HALO * nx + 2 * columns, nz)
    return call(lambda *refs: pack_y(columns, *refs), arrays(face, face), [VMEM], (field,), scratch=[(HALO * nx, nz)])


def call(kernel, out, inputs, operands, scratch=()):
    return pl.pallas_call(
        kernel,
        out_shape=out,
        in_specs=inputs,
        out_specs=(VMEM,) * len(out),
        scratch_shapes=[pltpu.VMEM(s, jnp.float32) for s in scratch],
        compiler_params=pltpu.CompilerParams(vmem_limit_bytes=16 * 1024 * 1024),
        cost_estimate=pl.CostEstimate(flops=5000000, bytes_accessed=1500000, transcendentals=0),
    )(*operands)


def line(count):
    return [(i, i + 1) for i in range(count - 1)]


def back(pairs):
    return [(b, a) for a, b in pairs]


def exchange(field, pair, columns):
    ny = field.shape[2]
    half = HALO * ny + 2 * columns
    count = lax.axis_size("gx")
    swapped = lax.ppermute(pair, "gx", [(i, i ^ 1) for i in range(count)])
    y_low, y_high = y_faces(field, columns)
    up = line(lax.axis_size("gy"))
    from_y_low = lax.ppermute(y_high, "gy", up)
    from_y_high = lax.ppermute(y_low, "gy", back(up))
    onward = [(i, (i + 2 - 4 * (i % 2)) % count) for i in range(count)]
    outer = lax.ppermute(swapped[half:], "gx", onward)
    return swapped[:half], outer, from_y_low, from_y_high


def per_device(pressure_now, pressure_before, region_code, velocity, wavelet, source_cell):
    shape = pressure_now.shape
    nx, ny, nz = shape
    field = (2,) + shape
    grid_y = ny * lax.axis_size("gy")
    grid_z = nz * lax.axis_size("gz")
    x = source_cell // (grid_y * grid_z) - lax.axis_index("gx") * nx
    y = source_cell // grid_z % grid_y - lax.axis_index("gy") * ny
    z = source_cell % grid_z - lax.axis_index("gz") * nz
    inside = (x >= 0) & (x < nx) & (y >= 0) & (y < ny) & (z >= -DEEP) & (z < nz + DEEP)
    place = jnp.where(z < 0, z + 2 * nz, z)
    cells = jnp.where(inside, (((place // nz) * nx + x) * ny + y) * nz + place % nz, -1)
    cells = jnp.broadcast_to(cells[:, None], (cells.shape[0], nz))
    amounts = [jnp.broadcast_to(wavelet[step][:, None], (wavelet.shape[1], nz)) for step in range(STEPS)]

    deep = (3 * DEEP, nx * ny)
    in_hbm = pl.BlockSpec(memory_space=pltpu.HBM)
    rate, z_low, z_high = pl.pallas_call(
        first_kernel,
        out_shape=arrays(shape, deep, deep),
        in_specs=[in_hbm] * 4,
        out_specs=(VMEM,) * 3,
        scratch_shapes=[
            pltpu.SMEM(velocity.shape, jnp.float32),
            pltpu.VMEM(shape, jnp.float32),
            pltpu.VMEM(shape, jnp.float32),
            pltpu.VMEM(shape, jnp.int32),
            pltpu.SemaphoreType.DMA((4,)),
        ],
        compiler_params=pltpu.CompilerParams(vmem_limit_bytes=16 * 1024 * 1024),
        cost_estimate=pl.CostEstimate(flops=5000000, bytes_accessed=1500000, transcendentals=0),
        name="first",
    )(*(pltpu.with_memory_space_constraint(a, pltpu.HBM) for a in (velocity, pressure_now, pressure_before, region_code)))
    up = line(lax.axis_size("gz"))
    from_low = lax.ppermute(z_high, "gz", up)
    from_high = lax.ppermute(z_low, "gz", back(up))
    current, pair = call(
        widen_now, arrays(field, pair_shape(shape, extra(0))), [VMEM] * 3, (pressure_now, from_low, from_high)
    )
    before, rate = call(widen_rest, arrays(field, field), [VMEM] * 4, (pressure_before, rate, from_low, from_high))
    for step in range(STEPS):
        last = step == STEPS - 1
        inner, outer, y_low, y_high = exchange(current, pair, extra(step))
        early = call(
            lambda *refs, step=step: part_zero(step, *refs),
            arrays(shape, shape) if last else arrays(field),
            [VMEM] * 3,
            (current, before, rate),
            scratch=[(2, nx, ny + 16, nz)],
        )
        out = call(
            lambda *refs, step=step: part_one(step, *refs),
            arrays(shape) if last else arrays(field, face_shape(shape, extra(step + 1))),
            [VMEM] * 7,
            (early[0], rate, cells, amounts[step], inner, y_low, y_high),
            scratch=[(2, HALO, ny, nz), (2, 2, nx, 16, nz)],
        )
        partial = out[0]
        following, *pairs = call(
            lambda *refs, step=step: part_two(step, *refs),
            arrays(shape) if last else arrays(field, pair_shape(shape, extra(step + 1))),
            [VMEM] * (3 if last else 4),
            (partial, rate, outer) if last else (partial, rate, outer, out[1]),
            scratch=[(2, HALO, ny, nz)],
        )
        pair = pairs[0] if pairs else None
        before, current = (early[1], following) if last else (current, following)
    return current, before


def solution(mesh):
    field = P("gx", "gy", "gz")
    return jax.shard_map(
        per_device,
        mesh=mesh,
        in_specs=(field, field, field, P(), P(), P()),
        out_specs=(field, field),
        check_vma=False,
    )
```
